32 devices in a mesh: rep: 2 (over x), shard: 16 (over z, y, core).
Axes of the slice: x: 2, y: 2, z: 4, core: 2. Of those that a mesh axis runs over, the one named last changes fastest.
Arguments:
- ratings_a: float32 [2048, 16384], P(('rep', 'shard')), parts along dimension 0
- mask_a: int32 [2048, 16384], P(('rep', 'shard')), parts along dimension 0
- users_a: float32 [2048, 32], P(('rep', 'shard')), parts along dimension 0
- items_a: float32 [32768, 32], P(('rep', 'shard')), parts along dimension 0
- ratings_b: float32 [2048, 16384], P(('rep', 'shard')), parts along dimension 0
- mask_b: int32 [2048, 16384], P(('rep', 'shard')), parts along dimension 0
- users_b: float32 [2048, 32], P(('rep', 'shard')), parts along dimension 0
- items_b: float32 [32768, 32], P(('rep', 'shard')), parts along dimension 0
Outputs:
- output 1: float32 [2048, 32], P(('rep', 'shard')), parts along dimension 0
- output 2: float32 [32768, 32], P(('rep', 'shard')), parts along dimension 0
- output 3: float32 [2048, 32], P(('rep', 'shard')), parts along dimension 0
- output 4: float32 [32768, 32], P(('rep', 'shard')), parts along dimension 0
There are 2 independent parts. The reference program is written for one: setup_inputs(seed, part) draws one part's arguments, and reference() takes and returns one part's arrays. A program takes and returns all parts, laid end to end along the dimension named above; each array names one.
All inputs are finite; a program needn't handle non-finite values.
Results may differ from the reference program's by a relative error of at most 0.00331626.
Values are sent between devices in bfloat16 or wider.
A program may use at most 1 GiB of HBM per device.

```python
import math
import jax
import jax.numpy as jnp
from jax import lax

SHARDS = 16
USERS_DEV = 64
ITEMS = 16384
RANK = 32
SWEEP_STEPS = 4
EPOCHS = 2
WEIGHT_DECAY = 0.05
USERS = SHARDS * USERS_DEV
ITEM_BLOCK = ITEMS // SHARDS
STEP_U = 0.5 * math.sqrt(RANK) / (ITEM_BLOCK + 2 * RANK)
STEP_V = 0.5 * math.sqrt(RANK) / (USERS_DEV + 2 * RANK)


def draw_market(key):
    key_list = jax.random.split(key, 7)
    true_u = jax.random.normal(key_list[0], (USERS, RANK), jnp.float32)
    true_v = jax.random.normal(key_list[1], (ITEMS, RANK), jnp.float32)
    noise_draw = jax.random.normal(key_list[2], (USERS, ITEMS), jnp.float32)
    ratings = jnp.dot(true_u, true_v.T) / math.sqrt(RANK) + 0.3 * noise_draw
    user_rate = jax.random.randint(key_list[3], (USERS, 1), 10, 51)
    obs_mask = (jax.random.randint(key_list[4], (USERS, ITEMS), 0, 100) < user_rate).astype(jnp.int32)
    user_init = jax.random.normal(key_list[5], (USERS, RANK), jnp.float32) * RANK ** -0.25
    item_init = jax.random.normal(key_list[6], (ITEMS, RANK), jnp.float32) * RANK ** -0.25
    return ratings, obs_mask, user_init, item_init


def setup_inputs(seed: int = 0, part: int = 0) -> dict:
    base_key = jax.random.fold_in(jax.random.key(seed), part)
    rate_a, mask_a, user_a, item_a = draw_market(jax.random.fold_in(base_key, 1))
    rate_b, mask_b, user_b, item_b = draw_market(jax.random.fold_in(base_key, 2))
    return {"ratings_a": rate_a, "mask_a": mask_a, "users_a": user_a, "items_a": item_a, "ratings_b": rate_b, "mask_b": mask_b, "users_b": user_b, "items_b": item_b}


def factorize_market(ratings, obs_mask, user_init, item_init):
    rate_blocks = ratings.reshape(SHARDS, USERS_DEV, SHARDS, ITEM_BLOCK)
    flag_blocks = obs_mask.reshape(SHARDS, USERS_DEV, SHARDS, ITEM_BLOCK).astype(jnp.float32)
    shard_ids = jnp.arange(SHARDS)

    def sub_epoch(carry_state, hop_index):
        user_blocks, held_items = carry_state
        col_ids = (shard_ids + hop_index) % SHARDS
        rate_now = rate_blocks[shard_ids, :, col_ids, :]
        flag_now = flag_blocks[shard_ids, :, col_ids, :]

        def gradient_step(step_state, unused):
            user_cur, item_cur = step_state
            user_low = user_cur.astype(jnp.bfloat16).astype(jnp.float32)
            item_low = item_cur.astype(jnp.bfloat16).astype(jnp.float32)
            approx = jnp.einsum("pur,pvr->puv", user_low, item_low)
            err_low = (flag_now * (approx - rate_now)).astype(jnp.bfloat16).astype(jnp.float32)
            grad_u = jnp.einsum("puv,pvr->pur", err_low, item_low) + WEIGHT_DECAY * user_cur
            grad_v = jnp.einsum("puv,pur->pvr", err_low, user_low) + WEIGHT_DECAY * item_cur
            return (user_cur - STEP_U * grad_u, item_cur - STEP_V * grad_v), None

        (user_blocks, held_items), unused_out = lax.scan(gradient_step, (user_blocks, held_items), None, length=SWEEP_STEPS)
        return (user_blocks, jnp.roll(held_items, -1, axis=0)), None

    hop_list = jnp.tile(jnp.arange(SHARDS), EPOCHS)
    start_state = (user_init.reshape(SHARDS, USERS_DEV, RANK), item_init.reshape(SHARDS, ITEM_BLOCK, RANK))
    (user_blocks, held_items), unused_out = lax.scan(sub_epoch, start_state, hop_list)
    return user_blocks.reshape(USERS, RANK), held_items.reshape(ITEMS, RANK)


def reference(ratings_a, mask_a, users_a, items_a, ratings_b, mask_b, users_b, items_b):
    user_out_a, item_out_a = factorize_market(ratings_a, mask_a, users_a, items_a)
    user_out_b, item_out_b = factorize_market(ratings_b, mask_b, users_b, items_b)
    return (user_out_a, item_out_a, user_out_b, item_out_b)
```

```python
import functools
import math
import jax
import jax.numpy as jnp
from jax import lax
from jax.experimental import pallas as pl
from jax.experimental.pallas import tpu as pltpu
from jax.sharding import PartitionSpec as P

SWEEP_STEPS = 4
EPOCHS = 2
WEIGHT_DECAY = 0.05
CHUNK = 256
MESH = pl.DeviceIdType.MESH


def sweep(u_ref, v_ref, rate_ref, flag_ref, step_u, step_v):
    user = u_ref[...]
    user_low = user.astype(jnp.bfloat16)
    user_low_t = user.T.astype(jnp.bfloat16)
    grad_u = None
    for c in range(v_ref.shape[0]):
        cols = pl.ds(c * CHUNK, CHUNK)
        item = v_ref[c]
        item_low = item.astype(jnp.bfloat16)
        approx = jnp.dot(user_low, item_low, preferred_element_type=jnp.float32)
        err_low = (approx - rate_ref[:, cols]).astype(jnp.bfloat16) * flag_ref[:, cols]
        part = lax.dot_general(err_low, item_low, (((1,), (1,)), ((), ())), preferred_element_type=jnp.float32)
        grad_u = part if grad_u is None else grad_u + part
        grad_v = jnp.dot(user_low_t, err_low, preferred_element_type=jnp.float32)
        v_ref[c] = item - step_v * (grad_v + WEIGHT_DECAY * item)
    u_ref[...] = user - step_u * (grad_u + WEIGHT_DECAY * user)


def kernel(shards, step_u, step_v, ra, ma, ua, va, rb, mb, ub, vb, ua_o, va_o, ub_o, vb_o,
           rates, masks, flags, items, users, load_sem, first_sem, send_sem, recv_sem, out_sem):
    me = lax.axis_index("shard")
    left = lax.rem(me + shards - 1, shards)
    right = lax.rem(me + 1, shards)
    block = rates.shape[-1]
    chunks = block // CHUNK
    stages = EPOCHS * shards
    rate_in, mask_in = (ra, rb), (ma, mb)

    def loads(m, t):
        j = lax.rem(me + t, shards)
        cols = pl.ds(pl.multiple_of(j * block, block), block)
        return (pltpu.make_async_copy(rate_in[m].at[:, cols], rates.at[m, j], load_sem.at[0, m, j]),
                pltpu.make_async_copy(mask_in[m].at[:, cols], masks.at[m, j], load_sem.at[1, m, j]))

    def first(m, c):
        return pltpu.make_async_copy((va, vb)[m].at[:, pl.ds(c * CHUNK, CHUNK)], items.at[m, 0, c], first_sem.at[m, c])

    def last(m, c):
        return pltpu.make_async_copy(items.at[m, stages, c], (va_o, vb_o)[m].at[:, pl.ds(c * CHUNK, CHUNK)], out_sem.at[m, c])

    def hop(m, t):
        return pltpu.make_async_remote_copy(
            src_ref=items.at[m, t], dst_ref=items.at[m, t + 1], send_sem=send_sem.at[m],
            recv_sem=recv_sem.at[m, t + 1], device_id={"shard": left}, device_id_type=MESH)

    for m in range(2):
        for c in range(chunks):
            first(m, c).start()
        for cp in loads(m, 0):
            cp.start()

    barrier = pltpu.get_barrier_semaphore()
    for other in (left, right):
        pl.semaphore_signal(barrier, inc=1, device_id={"shard": other}, device_id_type=MESH)

    @pl.loop(1, shards)
    def _(t):
        for m in range(2):
            for cp in loads(m, t):
                cp.start()

    users[0] = ua[...].T
    users[1] = ub[...].T
    for m in range(2):
        for c in range(chunks):
            first(m, c).wait()
    pl.semaphore_wait(barrier, 2)

    @pl.loop(0, stages)
    def _(t):
        j = lax.rem(me + t, shards)
        for m in range(2):
            @pl.when(t < shards)
            def _():
                for cp in loads(m, t):
                    cp.wait()
            flags[m] = masks[m, j].astype(jnp.float32).astype(jnp.bfloat16)

            @pl.when(t > 0)
            def _():
                hop(m, t - 1).wait()

            @pl.loop(0, SWEEP_STEPS)
            def _(s):
                sweep(users.at[m], items.at[m, t], rates.at[m, j], flags.at[m], step_u, step_v)
            hop(m, t).start()

    ua_o[...] = users[0].T
    ub_o[...] = users[1].T
    for m in range(2):
        hop(m, stages - 1).wait()
        for c in range(chunks):
            last(m, c).start()
    for m in range(2):
        for c in range(chunks):
            last(m, c).wait()


def solution(mesh):
    shards = mesh.shape["shard"]
    row_spec = P(("rep", "shard"), None)

    def device_body(ratings_a, mask_a, users_a, items_a, ratings_b, mask_b, users_b, items_b):
        users_dev, rank = users_a.shape
        block = items_a.shape[0]
        chunks = block // CHUNK
        stages = EPOCHS * shards
        step_u = 0.5 * math.sqrt(rank) / (block + 2 * rank)
        step_v = 0.5 * math.sqrt(rank) / (users_dev + 2 * rank)
        hbm = pl.BlockSpec(memory_space=pl.ANY)
        vmem = pl.BlockSpec(memory_space=pltpu.VMEM)
        f32 = jnp.float32
        ut = jax.ShapeDtypeStruct((rank, users_dev), f32)
        vt = jax.ShapeDtypeStruct((rank, block), f32)
        outs = pl.pallas_call(
            functools.partial(kernel, shards, step_u, step_v),
            out_shape=(ut, vt, ut, vt),
            in_specs=[hbm, hbm, vmem, hbm] * 2,
            out_specs=[vmem, hbm] * 2,
            scratch_shapes=[
                pltpu.VMEM((2, shards, users_dev, block), f32),
                pltpu.VMEM((2, shards, users_dev, block), jnp.int32),
                pltpu.VMEM((2, users_dev, block), jnp.bfloat16),
                pltpu.VMEM((2, stages + 1, chunks, rank, CHUNK), f32),
                pltpu.VMEM((2, users_dev, rank), f32),
                pltpu.SemaphoreType.DMA((2, 2, shards)),
                pltpu.SemaphoreType.DMA((2, chunks)),
                pltpu.SemaphoreType.DMA((2,)),
                pltpu.SemaphoreType.DMA((2, stages + 1)),
                pltpu.SemaphoreType.DMA((2, chunks)),
            ],
            compiler_params=pltpu.CompilerParams(
                collective_id=0, has_side_effects=True, vmem_limit_bytes=48 * 1024 * 1024),
            name="sweep_ring",
        )(ratings_a, mask_a, users_a.T, items_a.T, ratings_b, mask_b, users_b.T, items_b.T)
        return tuple(o.T for o in outs)

    return jax.shard_map(device_body, mesh=mesh, in_specs=(row_spec,) * 8, out_specs=(row_spec,) * 4, check_vma=False)
```

```python
import functools
import math
import jax
import jax.numpy as jnp
from jax import lax
from jax.experimental import pallas as pl
from jax.experimental.pallas import tpu as pltpu
from jax.sharding import PartitionSpec as P

SWEEP_STEPS = 4
EPOCHS = 2
WEIGHT_DECAY = 0.05
CHUNK = 256
MESH = pl.DeviceIdType.MESH


def sweep(u_ref, v_ref, rate_ref, flag_ref, step_u, step_v):
    user = u_ref[...]
    user_low = user.astype(jnp.bfloat16)
    user_low_t = user.T.astype(jnp.bfloat16)
    grad_u = None
    for c in range(v_ref.shape[0]):
        cols = pl.ds(c * CHUNK, CHUNK)
        item = v_ref[c]
        item_low = item.astype(jnp.bfloat16)
        approx = jnp.dot(user_low, item_low, preferred_element_type=jnp.float32)
        err_low = (approx - rate_ref[:, cols]).astype(jnp.bfloat16) * flag_ref[:, cols]
        part = lax.dot_general(err_low, item_low, (((1,), (1,)), ((), ())), preferred_element_type=jnp.float32)
        grad_u = part if grad_u is None else grad_u + part
        grad_v = jnp.dot(user_low_t, err_low, preferred_element_type=jnp.float32)
        v_ref[c] = item - step_v * (grad_v + WEIGHT_DECAY * item)
    u_ref[...] = user - step_u * (grad_u + WEIGHT_DECAY * user)


def kernel(shards, step_u, step_v, ra, ma, ua, va, rb, mb, ub, vb, ua_o, va_o, ub_o, vb_o,
           rates, masks, flags, items, users, load_sem, first_sem, send_sem, recv_sem, out_sem):
    me = lax.axis_index("shard")
    left = lax.rem(me + shards - 1, shards)
    right = lax.rem(me + 1, shards)
    block = rates.shape[-1]
    chunks = block // CHUNK
    stages = EPOCHS * shards
    rate_in, mask_in = (ra, rb), (ma, mb)

    def loads(m, t):
        j = lax.rem(me + t, shards)
        cols = pl.ds(pl.multiple_of(j * block, block), block)
        return (pltpu.make_async_copy(rate_in[m].at[:, cols], rates.at[m, j], load_sem.at[0, m, j]),
                pltpu.make_async_copy(mask_in[m].at[:, cols], masks.at[m, j], load_sem.at[1, m, j]))

    def first(m, c):
        return pltpu.make_async_copy((va, vb)[m].at[:, pl.ds(c * CHUNK, CHUNK)], items.at[m, 0, c], first_sem.at[m, c])

    def last(m, c):
        return pltpu.make_async_copy(items.at[m, stages, c], (va_o, vb_o)[m].at[:, pl.ds(c * CHUNK, CHUNK)], out_sem.at[m, c])

    def hop(m, t):
        return pltpu.make_async_remote_copy(
            src_ref=items.at[m, t], dst_ref=items.at[m, t + 1], send_sem=send_sem.at[m, t],
            recv_sem=recv_sem.at[m, t + 1], device_id={"shard": left}, device_id_type=MESH)

    for m in range(2):
        for c in range(chunks):
            first(m, c).start()
        for cp in loads(m, 0):
            cp.start()

    barrier = pltpu.get_barrier_semaphore()
    for other in (left, right):
        pl.semaphore_signal(barrier, inc=1, device_id={"shard": other}, device_id_type=MESH)

    @pl.loop(1, shards)
    def _(t):
        for m in range(2):
            for cp in loads(m, t):
                cp.start()

    users[0] = ua[...].T
    users[1] = ub[...].T
    for m in range(2):
        for c in range(chunks):
            first(m, c).wait()
    pl.semaphore_wait(barrier, 2)

    @pl.loop(0, stages)
    def _(t):
        j = lax.rem(me + t, shards)
        for m in range(2):
            @pl.when(t < shards)
            def _():
                for cp in loads(m, t):
                    cp.wait()
            flags[m] = masks[m, j].astype(jnp.float32).astype(jnp.bfloat16)

            @pl.when(t > 0)
            def _():
                hop(m, t - 1).wait_recv()

            @pl.loop(0, SWEEP_STEPS)
            def _(s):
                sweep(users.at[m], items.at[m, t], rates.at[m, j], flags.at[m], step_u, step_v)
            hop(m, t).start()

    ua_o[...] = users[0].T
    ub_o[...] = users[1].T
    for m in range(2):
        hop(m, stages - 1).wait_recv()
        for c in range(chunks):
            last(m, c).start()
    for m in range(2):
        for c in range(chunks):
            last(m, c).wait()

    @pl.loop(0, stages)
    def _(t):
        for m in range(2):
            hop(m, t).wait_send()


def solution(mesh):
    shards = mesh.shape["shard"]
    row_spec = P(("rep", "shard"), None)

    def device_body(ratings_a, mask_a, users_a, items_a, ratings_b, mask_b, users_b, items_b):
        users_dev, rank = users_a.shape
        block = items_a.shape[0]
        chunks = block // CHUNK
        stages = EPOCHS * shards
        step_u = 0.5 * math.sqrt(rank) / (block + 2 * rank)
        step_v = 0.5 * math.sqrt(rank) / (users_dev + 2 * rank)
        hbm = pl.BlockSpec(memory_space=pltpu.HBM)
        vmem = pl.BlockSpec(memory_space=pltpu.VMEM)
        f32 = jnp.float32
        ut = jax.ShapeDtypeStruct((rank, users_dev), f32)
        vt = jax.ShapeDtypeStruct((rank, block), f32)
        outs = pl.pallas_call(
            functools.partial(kernel, shards, step_u, step_v),
            out_shape=(ut, vt, ut, vt),
            in_specs=[hbm, hbm, vmem, hbm] * 2,
            out_specs=[vmem, hbm] * 2,
            scratch_shapes=[
                pltpu.VMEM((2, shards, users_dev, block), f32),
                pltpu.VMEM((2, shards, users_dev, block), jnp.int32),
                pltpu.VMEM((2, users_dev, block), jnp.bfloat16),
                pltpu.VMEM((2, stages + 1, chunks, rank, CHUNK), f32),
                pltpu.VMEM((2, users_dev, rank), f32),
                pltpu.SemaphoreType.DMA((2, 2, shards)),
                pltpu.SemaphoreType.DMA((2, chunks)),
                pltpu.SemaphoreType.DMA((2, stages)),
                pltpu.SemaphoreType.DMA((2, stages + 1)),
                pltpu.SemaphoreType.DMA((2, chunks)),
            ],
            compiler_params=pltpu.CompilerParams(
                collective_id=0, has_side_effects=True, vmem_limit_bytes=48 * 1024 * 1024),
            name="sweep_ring",
        )(ratings_a, mask_a, users_a.T, items_a.T, ratings_b, mask_b, users_b.T, items_b.T)
        return tuple(o.T for o in outs)

    return jax.shard_map(device_body, mesh=mesh, in_specs=(row_spec,) * 8, out_specs=(row_spec,) * 4, check_vma=False)
```

```python
import functools
import math
import jax
import jax.numpy as jnp
from jax import lax
from jax.experimental import pallas as pl
from jax.experimental.pallas import tpu as pltpu
from jax.sharding import PartitionSpec as P

SWEEP_STEPS = 4
EPOCHS = 2
WEIGHT_DECAY = 0.05
CHUNK = 256
MESH = pl.DeviceIdType.MESH


def sweep(u_ref, v_ref, rate_ref, flag_ref, step_u, step_v):
    user = u_ref[...]
    user_low = user.astype(jnp.bfloat16)
    user_low_t = user.T.astype(jnp.bfloat16)
    grad_u = None
    for c in range(v_ref.shape[0]):
        cols = pl.ds(c * CHUNK, CHUNK)
        item = v_ref[c]
        item_low = item.astype(jnp.bfloat16)
        approx = jnp.dot(user_low, item_low, preferred_element_type=jnp.float32)
        err_low = (approx - rate_ref[:, cols]).astype(jnp.bfloat16) * flag_ref[:, cols]
        part = lax.dot_general(err_low, item_low, (((1,), (1,)), ((), ())), preferred_element_type=jnp.float32)
        grad_u = part if grad_u is None else grad_u + part
        grad_v = jnp.dot(user_low_t, err_low, preferred_element_type=jnp.float32)
        v_ref[c] = item - step_v * (grad_v + WEIGHT_DECAY * item)
    u_ref[...] = user - step_u * (grad_u + WEIGHT_DECAY * user)


def kernel(shards, step_u, step_v, ra, ma, ua, va, rb, mb, ub, vb, ua_o, va_o, ub_o, vb_o,
           rates, masks, flags, items, last_items, users, users_in, users_out,
           load_sem, push_sem, send_sem, recv_sem, last_sem, user_sem, out_sem):
    me = lax.axis_index("shard")
    core = lax.rem(me, 2)
    base = me - core
    peer = base + 1 - core
    block = rates.shape[-1]
    chunks = block // CHUNK
    stages = EPOCHS * shards

    def dev(index):
        return {"shard": lax.rem(index + shards, shards)}

    def own(k):
        return (ra, ma, ua, va) if k == 0 else (rb, mb, ub, vb)

    def span(j):
        return pl.ds(pl.multiple_of(j * block, block), block)

    def pieces(k, q):
        j = lax.rem(base + k + q, shards)
        out = []
        for kind, buf in ((0, rates), (1, masks)):
            out.append(pltpu.make_async_copy(own(k)[kind].at[:, span(j)], buf.at[k, j], load_sem.at[kind, k, j]))
            out.append(pltpu.make_async_remote_copy(
                src_ref=own(1 - k)[kind].at[:, span(j)], dst_ref=buf.at[k, j], send_sem=push_sem.at[kind, j],
                recv_sem=load_sem.at[kind, k, j], device_id=dev(peer), device_id_type=MESH))
        return out

    def firsts(k):
        out = []
        for c in range(chunks):
            cols = pl.ds(c * CHUNK, CHUNK)
            out.append((pltpu.make_async_copy(own(k)[3].at[:, cols], items.at[k, c], recv_sem.at[k]),
                        pltpu.make_async_remote_copy(
                            src_ref=own(1 - k)[3].at[:, cols], dst_ref=items.at[k, c], send_sem=last_sem.at[2],
                            recv_sem=recv_sem.at[k], device_id=dev(peer), device_id_type=MESH)))
        return out

    def user_push(k):
        return pltpu.make_async_remote_copy(
            src_ref=own(1 - k)[2], dst_ref=users_in, send_sem=user_sem.at[0], recv_sem=user_sem.at[1],
            device_id=dev(peer), device_id_type=MESH)

    def hop(s):
        return pltpu.make_async_remote_copy(
            src_ref=items.at[s], dst_ref=items.at[s + 2], send_sem=send_sem.at[s],
            recv_sem=recv_sem.at[s + 2], device_id=dev(me - 2), device_id_type=MESH)

    def home(s, target):
        return pltpu.make_async_remote_copy(
            src_ref=items.at[s], dst_ref=last_items.at[core], send_sem=send_sem.at[s],
            recv_sem=last_sem.at[core], device_id=dev(target), device_id_type=MESH)

    def user_home(k):
        return pltpu.make_async_remote_copy(
            src_ref=users.at[1 - k], dst_ref=users_out, send_sem=user_sem.at[2], recv_sem=user_sem.at[3],
            device_id=dev(peer), device_id_type=MESH)

    def landed(s):
        return pltpu.make_async_copy(items.at[s], items.at[s], recv_sem.at[s])

    barrier = pltpu.get_barrier_semaphore()
    for step in (-2, -1, 1, 2):
        pl.semaphore_signal(barrier, inc=1, device_id=dev(me + step), device_id_type=MESH)
    pl.semaphore_wait(barrier, 4)

    for k in range(2):
        @pl.when(core == k)
        def _():
            user_push(k).start()
            for here, there in firsts(k):
                here.start()
                there.start()
            users[k] = own(k)[2][...].T

            @pl.loop(0, shards)
            def _(q):
                for cp in pieces(k, q):
                    cp.start()

    for k in range(2):
        @pl.when(core == k)
        def _():
            user_push(k).wait_recv()
            users[1 - k] = users_in[...].T

    def ready(role, j):
        for kind, buf in ((0, rates), (1, masks)):
            pltpu.make_async_copy(buf.at[role, j], buf.at[role, j], load_sem.at[kind, role, j]).wait()

    def visit(role, s, j):
        @pl.loop(0, SWEEP_STEPS)
        def _(n):
            sweep(users.at[role], items.at[s], rates.at[role, j], flags.at[role], step_u, step_v)

    @pl.loop(0, stages + 1)
    def _(s):
        j = lax.rem(base + s, shards)

        @pl.when(s < shards)
        def _():
            ready(0, j)

        @pl.when(jnp.logical_and(s >= 1, s <= shards))
        def _():
            ready(1, j)

        flags[0] = masks[0, j].astype(jnp.float32).astype(jnp.bfloat16)

        @pl.when(s > 0)
        def _():
            flags[1] = masks[1, j].astype(jnp.float32).astype(jnp.bfloat16)

        landed(s).wait()

        @pl.when(s > 0)
        def _():
            visit(1, s, j)

        @pl.when(s < stages)
        def _():
            visit(0, s, j)

        @pl.when(s < stages - 1)
        def _():
            hop(s).start()

        @pl.when(s == stages - 1)
        def _():
            home(s, base - 1).start()

    for k in range(2):
        @pl.when(core == k)
        def _():
            user_home(k).start()
            (ua_o, ub_o)[k][...] = users[k].T

    @pl.when(core == 1)
    def _():
        home(stages, base).start()

    def outs(k):
        got = []
        for m in range(2):
            src = items.at[stages] if (k == 0 and m == 0) else last_items.at[m]
            for c in range(chunks):
                got.append(pltpu.make_async_copy(src.at[c], (va_o, vb_o)[m].at[:, pl.ds(c * CHUNK, CHUNK)], out_sem.at[m, c]))
        return got

    for k in range(2):
        @pl.when(core == k)
        def _():
            for m in range(2):
                if k or m:
                    pltpu.make_async_copy(last_items.at[m], last_items.at[m], last_sem.at[m]).wait()
            for cp in outs(k):
                cp.start()
            user_home(k).wait()
            (ua_o, ub_o)[1 - k][...] = users_out[...].T
            for cp in outs(k):
                cp.wait()
            user_push(k).wait_send()
            pltpu.make_async_copy(items.at[k], items.at[k], last_sem.at[2]).wait()

            @pl.loop(0, shards)
            def _(q):
                for cp in pieces(k, q)[1::2]:
                    cp.wait_send()

    @pl.loop(0, stages)
    def _(s):
        pltpu.make_async_copy(items.at[s], items.at[s], send_sem.at[s]).wait()

    @pl.when(core == 1)
    def _():
        home(stages, base).wait_send()


def solution(mesh):
    shards = mesh.shape["shard"]
    row_spec = P(("rep", "shard"), None)

    def device_body(ratings_a, mask_a, users_a, items_a, ratings_b, mask_b, users_b, items_b):
        users_dev, rank = users_a.shape
        block = items_a.shape[0]
        chunks = block // CHUNK
        stages = EPOCHS * shards
        step_u = 0.5 * math.sqrt(rank) / (block + 2 * rank)
        step_v = 0.5 * math.sqrt(rank) / (users_dev + 2 * rank)
        hbm = pl.BlockSpec(memory_space=pltpu.HBM)
        vmem = pl.BlockSpec(memory_space=pltpu.VMEM)
        f32 = jnp.float32
        ut = jax.ShapeDtypeStruct((rank, users_dev), f32)
        vt = jax.ShapeDtypeStruct((rank, block), f32)
        outs = pl.pallas_call(
            functools.partial(kernel, shards, step_u, step_v),
            out_shape=(ut, vt, ut, vt),
            in_specs=[hbm, hbm, vmem, hbm] * 2,
            out_specs=[vmem, hbm] * 2,
            scratch_shapes=[
                pltpu.VMEM((2, shards, users_dev, block), f32),
                pltpu.VMEM((2, shards, users_dev, block), jnp.int32),
                pltpu.VMEM((2, users_dev, block), jnp.bfloat16),
                pltpu.VMEM((stages + 1, chunks, rank, CHUNK), f32),
                pltpu.VMEM((2, chunks, rank, CHUNK), f32),
                pltpu.VMEM((2, users_dev, rank), f32),
                pltpu.VMEM((rank, users_dev), f32),
                pltpu.VMEM((users_dev, rank), f32),
                pltpu.SemaphoreType.DMA((2, 2, shards)),
                pltpu.SemaphoreType.DMA((2, shards)),
                pltpu.SemaphoreType.DMA((stages + 1,)),
                pltpu.SemaphoreType.DMA((stages + 1,)),
                pltpu.SemaphoreType.DMA((3,)),
                pltpu.SemaphoreType.DMA((4,)),
                pltpu.SemaphoreType.DMA((2, chunks)),
            ],
            compiler_params=pltpu.CompilerParams(
                collective_id=0, has_side_effects=True, vmem_limit_bytes=62 * 1024 * 1024),
            name="sweep_ring",
        )(ratings_a, mask_a, users_a.T, items_a.T, ratings_b, mask_b, users_b.T, items_b.T)
        return tuple(o.T for o in outs)

    return jax.shard_map(device_body, mesh=mesh, in_specs=(row_spec,) * 8, out_specs=(row_spec,) * 4, check_vma=False)
```

```python
import functools
import math
import jax
import jax.numpy as jnp
from jax import lax
from jax.experimental import pallas as pl
from jax.experimental.pallas import tpu as pltpu
from jax.sharding import PartitionSpec as P

SWEEP_STEPS = 4
EPOCHS = 2
WEIGHT_DECAY = 0.05
CHUNK = 256
MESH = pl.DeviceIdType.MESH


def sweep(u_ref, v_ref, rate_ref, flag_ref, step_u, step_v):
    chunks = range(v_ref.shape[0])
    f32, bf16 = jnp.float32, jnp.bfloat16
    user = u_ref[...]
    user_low = user.astype(bf16)
    user_low_t = user.T.astype(bf16)
    item_low = [v_ref[c].astype(bf16) for c in chunks]
    approx = [jnp.dot(user_low, item_low[c], preferred_element_type=f32) for c in chunks]
    err_low = []
    for c in chunks:
        cols = pl.ds(c * CHUNK, CHUNK)
        err_low.append((approx[c] - rate_ref[:, cols]).astype(bf16) * flag_ref[:, cols])
    part = [lax.dot_general(err_low[c], item_low[c], (((1,), (1,)), ((), ())), preferred_element_type=f32) for c in chunks]
    grad_v = [jnp.dot(user_low_t, err_low[c], preferred_element_type=f32) for c in chunks]
    for c in chunks:
        item = v_ref[c]
        v_ref[c] = item - step_v * (grad_v[c] + WEIGHT_DECAY * item)
    grad_u = (part[0] + part[1]) + (part[2] + part[3])
    u_ref[...] = user - step_u * (grad_u + WEIGHT_DECAY * user)


def kernel(shards, step_u, step_v, ra, ma, ua, va, rb, mb, ub, vb, ua_o, va_o, ub_o, vb_o,
           rates, masks, flags, items, last_items, users, users_in, users_out,
           load_sem, push_sem, send_sem, recv_sem, last_sem, user_sem, out_sem):
    me = lax.axis_index("shard")
    core = lax.rem(me, 2)
    base = me - core
    peer = base + 1 - core
    block = rates.shape[-1]
    chunks = block // CHUNK
    stages = EPOCHS * shards

    def dev(index):
        return {"shard": lax.rem(index + shards, shards)}

    def own(k):
        return (ra, ma, ua, va) if k == 0 else (rb, mb, ub, vb)

    def span(j):
        return pl.ds(pl.multiple_of(j * block, block), block)

    def pieces(k, q):
        j = lax.rem(base + k + q, shards)
        out = []
        for kind, buf in ((0, rates), (1, masks)):
            out.append(pltpu.make_async_copy(own(k)[kind].at[:, span(j)], buf.at[k, j], load_sem.at[kind, k, j]))
            out.append(pltpu.make_async_remote_copy(
                src_ref=own(1 - k)[kind].at[:, span(j)], dst_ref=buf.at[k, j], send_sem=push_sem.at[kind, j],
                recv_sem=load_sem.at[kind, k, j], device_id=dev(peer), device_id_type=MESH))
        return out

    def firsts(k):
        out = []
        for c in range(chunks):
            cols = pl.ds(c * CHUNK, CHUNK)
            out.append((pltpu.make_async_copy(own(k)[3].at[:, cols], items.at[k, c], recv_sem.at[k]),
                        pltpu.make_async_remote_copy(
                            src_ref=own(1 - k)[3].at[:, cols], dst_ref=items.at[k, c], send_sem=last_sem.at[2],
                            recv_sem=recv_sem.at[k], device_id=dev(peer), device_id_type=MESH)))
        return out

    def user_push(k):
        return pltpu.make_async_remote_copy(
            src_ref=own(1 - k)[2], dst_ref=users_in, send_sem=user_sem.at[0], recv_sem=user_sem.at[1],
            device_id=dev(peer), device_id_type=MESH)

    def hop(s):
        return pltpu.make_async_remote_copy(
            src_ref=items.at[s], dst_ref=items.at[s + 2], send_sem=send_sem.at[s],
            recv_sem=recv_sem.at[s + 2], device_id=dev(me - 2), device_id_type=MESH)

    def home(s, target):
        return pltpu.make_async_remote_copy(
            src_ref=items.at[s], dst_ref=last_items.at[core], send_sem=send_sem.at[s],
            recv_sem=last_sem.at[core], device_id=dev(target), device_id_type=MESH)

    def user_home(k):
        return pltpu.make_async_remote_copy(
            src_ref=users.at[1 - k], dst_ref=users_out, send_sem=user_sem.at[2], recv_sem=user_sem.at[3],
            device_id=dev(peer), device_id_type=MESH)

    def landed(s):
        return pltpu.make_async_copy(items.at[s], items.at[s], recv_sem.at[s])

    barrier = pltpu.get_barrier_semaphore()
    for step in (-2, -1, 1, 2):
        pl.semaphore_signal(barrier, inc=1, device_id=dev(me + step), device_id_type=MESH)
    pl.semaphore_wait(barrier, 4)

    for k in range(2):
        @pl.when(core == k)
        def _():
            user_push(k).start()
            for here, there in firsts(k):
                here.start()
                there.start()
            users[k] = own(k)[2][...].T

            @pl.loop(0, shards)
            def _(q):
                for cp in pieces(k, q):
                    cp.start()

    for k in range(2):
        @pl.when(core == k)
        def _():
            user_push(k).wait_recv()
            users[1 - k] = users_in[...].T

    def ready(role, j):
        for kind, buf in ((0, rates), (1, masks)):
            pltpu.make_async_copy(buf.at[role, j], buf.at[role, j], load_sem.at[kind, role, j]).wait()

    def visit(role, s, j):
        @pl.loop(0, SWEEP_STEPS)
        def _(n):
            sweep(users.at[role], items.at[s], rates.at[role, j], flags.at[role], step_u, step_v)

    @pl.loop(0, stages + 1)
    def _(s):
        j = lax.rem(base + s, shards)

        @pl.when(s < shards)
        def _():
            ready(0, j)

        @pl.when(jnp.logical_and(s >= 1, s <= shards))
        def _():
            ready(1, j)

        flags[0] = masks[0, j].astype(jnp.float32).astype(jnp.bfloat16)

        @pl.when(s > 0)
        def _():
            flags[1] = masks[1, j].astype(jnp.float32).astype(jnp.bfloat16)

        landed(s).wait()

        @pl.when(s > 0)
        def _():
            visit(1, s, j)

        @pl.when(s < stages)
        def _():
            visit(0, s, j)

        @pl.when(s < stages - 1)
        def _():
            hop(s).start()

        @pl.when(s == stages - 1)
        def _():
            home(s, base - 1).start()

    for k in range(2):
        @pl.when(core == k)
        def _():
            user_home(k).start()
            (ua_o, ub_o)[k][...] = users[k].T

    @pl.when(core == 1)
    def _():
        home(stages, base).start()

    def outs(k):
        got = []
        for m in range(2):
            src = items.at[stages] if (k == 0 and m == 0) else last_items.at[m]
            for c in range(chunks):
                got.append(pltpu.make_async_copy(src.at[c], (va_o, vb_o)[m].at[:, pl.ds(c * CHUNK, CHUNK)], out_sem.at[m, c]))
        return got

    for k in range(2):
        @pl.when(core == k)
        def _():
            for m in range(2):
                if k or m:
                    pltpu.make_async_copy(last_items.at[m], last_items.at[m], last_sem.at[m]).wait()
            for cp in outs(k):
                cp.start()
            user_home(k).wait()
            (ua_o, ub_o)[1 - k][...] = users_out[...].T
            for cp in outs(k):
                cp.wait()
            user_push(k).wait_send()
            pltpu.make_async_copy(items.at[k], items.at[k], last_sem.at[2]).wait()

            @pl.loop(0, shards)
            def _(q):
                for cp in pieces(k, q)[1::2]:
                    cp.wait_send()

    @pl.loop(0, stages)
    def _(s):
        pltpu.make_async_copy(items.at[s], items.at[s], send_sem.at[s]).wait()

    @pl.when(core == 1)
    def _():
        home(stages, base).wait_send()


def solution(mesh):
    shards = mesh.shape["shard"]
    row_spec = P(("rep", "shard"), None)

    def device_body(ratings_a, mask_a, users_a, items_a, ratings_b, mask_b, users_b, items_b):
        users_dev, rank = users_a.shape
        block = items_a.shape[0]
        chunks = block // CHUNK
        stages = EPOCHS * shards
        step_u = 0.5 * math.sqrt(rank) / (block + 2 * rank)
        step_v = 0.5 * math.sqrt(rank) / (users_dev + 2 * rank)
        hbm = pl.BlockSpec(memory_space=pltpu.HBM)
        vmem = pl.BlockSpec(memory_space=pltpu.VMEM)
        f32 = jnp.float32
        ut = jax.ShapeDtypeStruct((rank, users_dev), f32)
        vt = jax.ShapeDtypeStruct((rank, block), f32)
        outs = pl.pallas_call(
            functools.partial(kernel, shards, step_u, step_v),
            out_shape=(ut, vt, ut, vt),
            in_specs=[hbm, hbm, vmem, hbm] * 2,
            out_specs=[vmem, hbm] * 2,
            scratch_shapes=[
                pltpu.VMEM((2, shards, users_dev, block), f32),
                pltpu.VMEM((2, shards, users_dev, block), jnp.int32),
                pltpu.VMEM((2, users_dev, block), jnp.bfloat16),
                pltpu.VMEM((stages + 1, chunks, rank, CHUNK), f32),
                pltpu.VMEM((2, chunks, rank, CHUNK), f32),
                pltpu.VMEM((2, users_dev, rank), f32),
                pltpu.VMEM((rank, users_dev), f32),
                pltpu.VMEM((users_dev, rank), f32),
                pltpu.SemaphoreType.DMA((2, 2, shards)),
                pltpu.SemaphoreType.DMA((2, shards)),
                pltpu.SemaphoreType.DMA((stages + 1,)),
                pltpu.SemaphoreType.DMA((stages + 1,)),
                pltpu.SemaphoreType.DMA((3,)),
                pltpu.SemaphoreType.DMA((4,)),
                pltpu.SemaphoreType.DMA((2, chunks)),
            ],
            compiler_params=pltpu.CompilerParams(
                collective_id=0, has_side_effects=True, vmem_limit_bytes=62 * 1024 * 1024),
            name="sweep_ring",
        )(ratings_a, mask_a, users_a.T, items_a.T, ratings_b, mask_b, users_b.T, items_b.T)
        return tuple(o.T for o in outs)

    return jax.shard_map(device_body, mesh=mesh, in_specs=(row_spec,) * 8, out_specs=(row_spec,) * 4, check_vma=False)
```

```python
import functools
import math
import jax
import jax.numpy as jnp
from jax import lax
from jax.experimental import pallas as pl
from jax.experimental.pallas import tpu as pltpu
from jax.sharding import PartitionSpec as P

SWEEP_STEPS = 4
EPOCHS = 2
WEIGHT_DECAY = 0.05
CHUNK = 256
AHEAD = 3
STAGGER = 1500
MESH = pl.DeviceIdType.MESH


def sweep(u_ref, v_ref, rate_ref, flag_ref, step_u, step_v):
    chunks = range(v_ref.shape[0])
    f32, bf16 = jnp.float32, jnp.bfloat16
    user = u_ref[...]
    user_low = user.astype(bf16)
    user_low_t = user.T.astype(bf16)
    item_low = [v_ref[c].astype(bf16) for c in chunks]
    approx = [jnp.dot(user_low, item_low[c], preferred_element_type=f32) for c in chunks]
    err_low = []
    for c in chunks:
        cols = pl.ds(c * CHUNK, CHUNK)
        err_low.append((approx[c] - rate_ref[:, cols]).astype(bf16) * flag_ref[:, cols])
    part = [lax.dot_general(err_low[c], item_low[c], (((1,), (1,)), ((), ())), preferred_element_type=f32) for c in chunks]
    grad_v = [jnp.dot(user_low_t, err_low[c], preferred_element_type=f32) for c in chunks]
    for c in chunks:
        item = v_ref[c]
        v_ref[c] = item - step_v * (grad_v[c] + WEIGHT_DECAY * item)
    grad_u = (part[0] + part[1]) + (part[2] + part[3])
    u_ref[...] = user - step_u * (grad_u + WEIGHT_DECAY * user)


def kernel(shards, step_u, step_v, ra, ma, ua, va, rb, mb, ub, vb, ua_o, va_o, ub_o, vb_o,
           rates, masks, flags, items, last_items, users, users_in, users_out,
           load_sem, push_sem, send_sem, recv_sem, last_sem, user_sem, out_sem):
    me = lax.axis_index("shard")
    core = lax.rem(me, 2)
    base = me - core
    peer = base + 1 - core
    block = rates.shape[-1]
    chunks = block // CHUNK
    stages = EPOCHS * shards

    def dev(index):
        return {"shard": lax.rem(index + shards, shards)}

    def own(k):
        return (ra, ma, ua, va) if k == 0 else (rb, mb, ub, vb)

    def span(j):
        return pl.ds(pl.multiple_of(j * block, block), block)

    def pieces(k, q):
        j = lax.rem(base + k + q, shards)
        out = []
        for kind, buf in ((0, rates), (1, masks)):
            out.append(pltpu.make_async_copy(own(k)[kind].at[:, span(j)], buf.at[k, j], load_sem.at[kind, k, j]))
            out.append(pltpu.make_async_remote_copy(
                src_ref=own(1 - k)[kind].at[:, span(j)], dst_ref=buf.at[k, j], send_sem=push_sem.at[kind, j],
                recv_sem=load_sem.at[kind, k, j], device_id=dev(peer), device_id_type=MESH))
        return out

    def firsts(k):
        out = []
        for c in range(chunks):
            cols = pl.ds(c * CHUNK, CHUNK)
            out.append((pltpu.make_async_copy(own(k)[3].at[:, cols], items.at[k, c], recv_sem.at[k]),
                        pltpu.make_async_remote_copy(
                            src_ref=own(1 - k)[3].at[:, cols], dst_ref=items.at[k, c], send_sem=last_sem.at[2],
                            recv_sem=recv_sem.at[k], device_id=dev(peer), device_id_type=MESH)))
        return out

    def user_push(k):
        return pltpu.make_async_remote_copy(
            src_ref=own(1 - k)[2], dst_ref=users_in, send_sem=user_sem.at[0], recv_sem=user_sem.at[1],
            device_id=dev(peer), device_id_type=MESH)

    def hop(s):
        return pltpu.make_async_remote_copy(
            src_ref=items.at[s], dst_ref=items.at[s + 2], send_sem=send_sem.at[s],
            recv_sem=recv_sem.at[s + 2], device_id=dev(me - 2), device_id_type=MESH)

    def home(s, target):
        return pltpu.make_async_remote_copy(
            src_ref=items.at[s], dst_ref=last_items.at[core], send_sem=send_sem.at[s],
            recv_sem=last_sem.at[core], device_id=dev(target), device_id_type=MESH)

    def user_home(k):
        return pltpu.make_async_remote_copy(
            src_ref=users.at[1 - k], dst_ref=users_out, send_sem=user_sem.at[2], recv_sem=user_sem.at[3],
            device_id=dev(peer), device_id_type=MESH)

    def landed(s):
        return pltpu.make_async_copy(items.at[s], items.at[s], recv_sem.at[s])

    barrier = pltpu.get_barrier_semaphore()
    for step in (-2, -1, 1, 2):
        pl.semaphore_signal(barrier, inc=1, device_id=dev(me + step), device_id_type=MESH)

    for k in range(2):
        @pl.when(core == k)
        def _():
            for here, there in firsts(k):
                here.start()
            for q in range(AHEAD):
                for cp in pieces(k, q)[0::2]:
                    cp.start()
            users[k] = own(k)[2][...].T

    pl.semaphore_wait(barrier, 4)

    for k in range(2):
        @pl.when(core == k)
        def _():
            user_push(k).start()
            for here, there in firsts(k):
                there.start()
            for q in range(AHEAD):
                for cp in pieces(k, q)[1::2]:
                    cp.start()

    for k in range(2):
        @pl.when(core == k)
        def _():
            user_push(k).wait_recv()
            users[1 - k] = users_in[...].T

    def ready(role, j):
        for kind, buf in ((0, rates), (1, masks)):
            pltpu.make_async_copy(buf.at[role, j], buf.at[role, j], load_sem.at[kind, role, j]).wait()

    def visit(role, s, j):
        @pl.loop(0, SWEEP_STEPS)
        def _(n):
            sweep(users.at[role], items.at[s], rates.at[role, j], flags.at[role], step_u, step_v)

    @pl.when(core == 1)
    def _():
        pl.delay(STAGGER)

    @pl.loop(0, stages + 1)
    def _(s):
        j = lax.rem(base + s, shards)

        for k in range(2):
            @pl.when(jnp.logical_and(core == k, s + AHEAD < shards))
            def _():
                for cp in pieces(k, s + AHEAD):
                    cp.start()

        @pl.when(s < shards)
        def _():
            ready(0, j)

        @pl.when(jnp.logical_and(s >= 1, s <= shards))
        def _():
            ready(1, j)

        flags[0] = masks[0, j].astype(jnp.float32).astype(jnp.bfloat16)

        @pl.when(s > 0)
        def _():
            flags[1] = masks[1, j].astype(jnp.float32).astype(jnp.bfloat16)

        landed(s).wait()

        @pl.when(s > 0)
        def _():
            visit(1, s, j)

        @pl.when(s < stages)
        def _():
            visit(0, s, j)

        @pl.when(s < stages - 1)
        def _():
            hop(s).start()

        @pl.when(s == stages - 1)
        def _():
            home(s, base - 1).start()

    for k in range(2):
        @pl.when(core == k)
        def _():
            user_home(k).start()
            (ua_o, ub_o)[k][...] = users[k].T

    @pl.when(core == 1)
    def _():
        home(stages, base).start()

    def outs(k):
        got = []
        for m in range(2):
            src = items.at[stages] if (k == 0 and m == 0) else last_items.at[m]
            for c in range(chunks):
                got.append(pltpu.make_async_copy(src.at[c], (va_o, vb_o)[m].at[:, pl.ds(c * CHUNK, CHUNK)], out_sem.at[m, c]))
        return got

    for k in range(2):
        @pl.when(core == k)
        def _():
            for m in range(2):
                if k or m:
                    pltpu.make_async_copy(last_items.at[m], last_items.at[m], last_sem.at[m]).wait()
            for cp in outs(k):
                cp.start()
            user_home(k).wait()
            (ua_o, ub_o)[1 - k][...] = users_out[...].T
            for cp in outs(k):
                cp.wait()
            user_push(k).wait_send()
            pltpu.make_async_copy(items.at[k], items.at[k], last_sem.at[2]).wait()

            @pl.loop(0, shards)
            def _(q):
                for cp in pieces(k, q)[1::2]:
                    cp.wait_send()

    @pl.loop(0, stages)
    def _(s):
        pltpu.make_async_copy(items.at[s], items.at[s], send_sem.at[s]).wait()

    @pl.when(core == 1)
    def _():
        home(stages, base).wait_send()


def place(ua, va, ub, vb, ua_o, va_o, ub_o, vb_o, sem):
    copies = [pltpu.make_async_copy(src, dst, sem.at[i])
              for i, (src, dst) in enumerate(((ua, ua_o), (va, va_o), (ub, ub_o), (vb, vb_o)))]
    for cp in copies:
        cp.start()
    for cp in copies:
        cp.wait()


def solution(mesh):
    shards = mesh.shape["shard"]
    row_spec = P(("rep", "shard"), None)

    def device_body(ratings_a, mask_a, users_a, items_a, ratings_b, mask_b, users_b, items_b):
        users_dev, rank = users_a.shape
        block = items_a.shape[0]
        chunks = block // CHUNK
        stages = EPOCHS * shards
        step_u = 0.5 * math.sqrt(rank) / (block + 2 * rank)
        step_v = 0.5 * math.sqrt(rank) / (users_dev + 2 * rank)
        hbm = pl.BlockSpec(memory_space=pltpu.HBM)
        vmem = pl.BlockSpec(memory_space=pltpu.VMEM)
        f32 = jnp.float32
        ut = jax.ShapeDtypeStruct((rank, users_dev), f32)
        vt = jax.ShapeDtypeStruct((rank, block), f32)
        outs = pl.pallas_call(
            functools.partial(kernel, shards, step_u, step_v),
            out_shape=(ut, vt, ut, vt),
            in_specs=[hbm, hbm, vmem, hbm] * 2,
            out_specs=[vmem] * 4,
            scratch_shapes=[
                pltpu.VMEM((2, shards, users_dev, block), f32),
                pltpu.VMEM((2, shards, users_dev, block), jnp.int32),
                pltpu.VMEM((2, users_dev, block), jnp.bfloat16),
                pltpu.VMEM((stages + 1, chunks, rank, CHUNK), f32),
                pltpu.VMEM((2, chunks, rank, CHUNK), f32),
                pltpu.VMEM((2, users_dev, rank), f32),
                pltpu.VMEM((rank, users_dev), f32),
                pltpu.VMEM((users_dev, rank), f32),
                pltpu.SemaphoreType.DMA((2, 2, shards)),
                pltpu.SemaphoreType.DMA((2, shards)),
                pltpu.SemaphoreType.DMA((stages + 1,)),
                pltpu.SemaphoreType.DMA((stages + 1,)),
                pltpu.SemaphoreType.DMA((3,)),
                pltpu.SemaphoreType.DMA((4,)),
                pltpu.SemaphoreType.DMA((2, chunks)),
            ],
            compiler_params=pltpu.CompilerParams(
                collective_id=0, has_side_effects=True, vmem_limit_bytes=60 * 1024 * 1024),
            name="sweep_ring",
        )(ratings_a, mask_a, users_a.T, items_a.T, ratings_b, mask_b, users_b.T, items_b.T)
        outs = pl.pallas_call(
            place,
            out_shape=(ut, vt, ut, vt),
            in_specs=[vmem] * 4,
            out_specs=[pl.BlockSpec(memory_space=pl.ANY)] * 4,
            scratch_shapes=[pltpu.SemaphoreType.DMA((4,))],
            compiler_params=pltpu.CompilerParams(vmem_limit_bytes=60 * 1024 * 1024),
            name="place",
        )(*outs)
        return tuple(o.T for o in outs)

    return jax.shard_map(device_body, mesh=mesh, in_specs=(row_spec,) * 8, out_specs=(row_spec,) * 4, check_vma=False)
```

```python
import functools
import math
import jax
import jax.numpy as jnp
from jax import lax
from jax.experimental import pallas as pl
from jax.experimental.pallas import tpu as pltpu
from jax.sharding import PartitionSpec as P

SWEEP_STEPS = 4
EPOCHS = 2
WEIGHT_DECAY = 0.05
CHUNK = 256
AHEAD = 3
MESH = pl.DeviceIdType.MESH


def sweep(u_ref, v_ref, rate_ref, flag_ref, step_u, step_v):
    chunks = range(v_ref.shape[0])
    f32, bf16 = jnp.float32, jnp.bfloat16
    user = u_ref[...]
    user_low = user.astype(bf16)
    user_low_t = user.T.astype(bf16)
    item_low = [v_ref[c].astype(bf16) for c in chunks]
    approx = [jnp.dot(user_low, item_low[c], preferred_element_type=f32) for c in chunks]
    err_low = []
    for c in chunks:
        cols = pl.ds(c * CHUNK, CHUNK)
        err_low.append((approx[c] - rate_ref[:, cols]).astype(bf16) * flag_ref[:, cols])
    part = [lax.dot_general(err_low[c], item_low[c], (((1,), (1,)), ((), ())), preferred_element_type=f32) for c in chunks]
    grad_v = [jnp.dot(user_low_t, err_low[c], preferred_element_type=f32) for c in chunks]
    for c in chunks:
        item = v_ref[c]
        v_ref[c] = item - step_v * (grad_v[c] + WEIGHT_DECAY * item)
    grad_u = (part[0] + part[1]) + (part[2] + part[3])
    u_ref[...] = user - step_u * (grad_u + WEIGHT_DECAY * user)


def kernel(shards, step_u, step_v, ra, ma, ua, va, rb, mb, ub, vb, ua_o, va_o, ub_o, vb_o,
           rates, masks, flags, items, last_items, users, users_in, users_out,
           load_sem, push_sem, send_sem, recv_sem, last_sem, user_sem, out_sem):
    me = lax.axis_index("shard")
    core = lax.rem(me, 2)
    base = me - core
    market = lax.rem(core + base // 2, 2)
    peer = base + 1 - core
    block = rates.shape[-1]
    chunks = block // CHUNK
    stages = EPOCHS * shards

    def dev(index):
        return {"shard": lax.rem(index + shards, shards)}

    def own(m):
        return (ra, ma, ua, va) if m == 0 else (rb, mb, ub, vb)

    def span(j):
        return pl.ds(pl.multiple_of(j * block, block), block)

    def pieces(m, q):
        j = lax.rem(base + core + q, shards)
        out = []
        for kind, buf in ((0, rates), (1, masks)):
            out.append(pltpu.make_async_copy(own(m)[kind].at[:, span(j)], buf.at[core, j], load_sem.at[kind, core, j]))
            out.append(pltpu.make_async_remote_copy(
                src_ref=own(1 - m)[kind].at[:, span(j)], dst_ref=buf.at[core, j], send_sem=push_sem.at[kind, j],
                recv_sem=load_sem.at[kind, core, j], device_id=dev(peer), device_id_type=MESH))
        return out

    def firsts(m):
        out = []
        for c in range(chunks):
            cols = pl.ds(c * CHUNK, CHUNK)
            out.append((pltpu.make_async_copy(own(m)[3].at[:, cols], items.at[core, c], recv_sem.at[core]),
                        pltpu.make_async_remote_copy(
                            src_ref=own(1 - m)[3].at[:, cols], dst_ref=items.at[core, c], send_sem=last_sem.at[2],
                            recv_sem=recv_sem.at[core], device_id=dev(peer), device_id_type=MESH)))
        return out

    def user_push(m):
        return pltpu.make_async_remote_copy(
            src_ref=own(1 - m)[2], dst_ref=users_in, send_sem=user_sem.at[0], recv_sem=user_sem.at[1],
            device_id=dev(peer), device_id_type=MESH)

    def hop(s):
        return pltpu.make_async_remote_copy(
            src_ref=items.at[s], dst_ref=items.at[s + 2], send_sem=send_sem.at[s],
            recv_sem=recv_sem.at[s + 2], device_id=dev(base - 1 - core), device_id_type=MESH)

    def home(s, target):
        return pltpu.make_async_remote_copy(
            src_ref=items.at[s], dst_ref=last_items.at[market], send_sem=send_sem.at[s],
            recv_sem=last_sem.at[market], device_id=dev(target), device_id_type=MESH)

    def user_home():
        return pltpu.make_async_remote_copy(
            src_ref=users.at[1 - core], dst_ref=users_out, send_sem=user_sem.at[2], recv_sem=user_sem.at[3],
            device_id=dev(peer), device_id_type=MESH)

    def landed(s):
        return pltpu.make_async_copy(items.at[s], items.at[s], recv_sem.at[s])

    barrier = pltpu.get_barrier_semaphore()
    for other in (base - 2, base - 1, peer, base + 2, base + 3):
        pl.semaphore_signal(barrier, inc=1, device_id=dev(other), device_id_type=MESH)

    for m in range(2):
        @pl.when(market == m)
        def _():
            for here, there in firsts(m):
                here.start()
            for q in range(AHEAD):
                for cp in pieces(m, q)[0::2]:
                    cp.start()
            users[core] = own(m)[2][...].T

    pl.semaphore_wait(barrier, 5)

    for m in range(2):
        @pl.when(market == m)
        def _():
            user_push(m).start()
            for here, there in firsts(m):
                there.start()
            for q in range(AHEAD):
                for cp in pieces(m, q)[1::2]:
                    cp.start()

    user_push(0).wait_recv()
    users[1 - core] = users_in[...].T

    def ready(role, j):
        for kind, buf in ((0, rates), (1, masks)):
            pltpu.make_async_copy(buf.at[role, j], buf.at[role, j], load_sem.at[kind, role, j]).wait()

    def visit(role, s, j):
        @pl.loop(0, SWEEP_STEPS)
        def _(n):
            sweep(users.at[role], items.at[s], rates.at[role, j], flags.at[role], step_u, step_v)

    @pl.loop(0, stages + 1)
    def _(s):
        j = lax.rem(base + s, shards)

        for m in range(2):
            @pl.when(jnp.logical_and(market == m, s + AHEAD < shards))
            def _():
                for cp in pieces(m, s + AHEAD):
                    cp.start()

        @pl.when(s < shards)
        def _():
            ready(0, j)

        @pl.when(jnp.logical_and(s >= 1, s <= shards))
        def _():
            ready(1, j)

        flags[0] = masks[0, j].astype(jnp.float32).astype(jnp.bfloat16)

        @pl.when(s > 0)
        def _():
            flags[1] = masks[1, j].astype(jnp.float32).astype(jnp.bfloat16)

        landed(s).wait()

        @pl.when(s > 0)
        def _():
            visit(1, s, j)

        @pl.when(s < stages)
        def _():
            visit(0, s, j)

        @pl.when(s < stages - 1)
        def _():
            hop(s).start()

        @pl.when(s == stages - 1)
        def _():
            home(s, base - 1).start()

    user_home().start()
    for m in range(2):
        @pl.when(market == m)
        def _():
            (ua_o, ub_o)[m][...] = users[core].T

    @pl.when(core == 1)
    def _():
        home(stages, base).start()

    def outs(src, m):
        return [pltpu.make_async_copy(src.at[c], (va_o, vb_o)[m].at[:, pl.ds(c * CHUNK, CHUNK)], out_sem.at[m, c])
                for c in range(chunks)]

    for m in range(2):
        mine = jnp.logical_and(core == 0, market == m)

        @pl.when(mine)
        def _():
            for cp in outs(items.at[stages], m):
                cp.start()

        @pl.when(jnp.logical_not(mine))
        def _():
            pltpu.make_async_copy(last_items.at[m], last_items.at[m], last_sem.at[m]).wait()
            for cp in outs(last_items.at[m], m):
                cp.start()

    user_home().wait()
    for m in range(2):
        @pl.when(market == m)
        def _():
            (ua_o, ub_o)[1 - m][...] = users_out[...].T
    for m in range(2):
        for cp in outs(last_items.at[m], m):
            cp.wait()
    user_push(0).wait_send()
    pltpu.make_async_copy(items.at[core], items.at[core], last_sem.at[2]).wait()

    @pl.loop(0, shards)
    def _(j):
        for kind, buf in ((0, rates), (1, masks)):
            pltpu.make_async_copy(buf.at[core, j], buf.at[core, j], push_sem.at[kind, j]).wait()

    @pl.loop(0, stages)
    def _(s):
        pltpu.make_async_copy(items.at[s], items.at[s], send_sem.at[s]).wait()

    @pl.when(core == 1)
    def _():
        home(stages, base).wait_send()


def place(ua, va, ub, vb, ua_o, va_o, ub_o, vb_o, sem):
    copies = [pltpu.make_async_copy(src, dst, sem.at[i])
              for i, (src, dst) in enumerate(((ua, ua_o), (va, va_o), (ub, ub_o), (vb, vb_o)))]
    for cp in copies:
        cp.start()
    for cp in copies:
        cp.wait()


def solution(mesh):
    shards = mesh.shape["shard"]
    row_spec = P(("rep", "shard"), None)

    def device_body(ratings_a, mask_a, users_a, items_a, ratings_b, mask_b, users_b, items_b):
        users_dev, rank = users_a.shape
        block = items_a.shape[0]
        chunks = block // CHUNK
        stages = EPOCHS * shards
        step_u = 0.5 * math.sqrt(rank) / (block + 2 * rank)
        step_v = 0.5 * math.sqrt(rank) / (users_dev + 2 * rank)
        hbm = pl.BlockSpec(memory_space=pltpu.HBM)
        vmem = pl.BlockSpec(memory_space=pltpu.VMEM)
        f32 = jnp.float32
        ut = jax.ShapeDtypeStruct((rank, users_dev), f32)
        vt = jax.ShapeDtypeStruct((rank, block), f32)
        outs = pl.pallas_call(
            functools.partial(kernel, shards, step_u, step_v),
            out_shape=(ut, vt, ut, vt),
            in_specs=[hbm, hbm, vmem, hbm] * 2,
            out_specs=[vmem] * 4,
            scratch_shapes=[
                pltpu.VMEM((2, shards, users_dev, block), f32),
                pltpu.VMEM((2, shards, users_dev, block), jnp.int32),
                pltpu.VMEM((2, users_dev, block), jnp.bfloat16),
                pltpu.VMEM((stages + 1, chunks, rank, CHUNK), f32),
                pltpu.VMEM((2, chunks, rank, CHUNK), f32),
                pltpu.VMEM((2, users_dev, rank), f32),
                pltpu.VMEM((rank, users_dev), f32),
                pltpu.VMEM((users_dev, rank), f32),
                pltpu.SemaphoreType.DMA((2, 2, shards)),
                pltpu.SemaphoreType.DMA((2, shards)),
                pltpu.SemaphoreType.DMA((stages + 1,)),
                pltpu.SemaphoreType.DMA((stages + 1,)),
                pltpu.SemaphoreType.DMA((3,)),
                pltpu.SemaphoreType.DMA((4,)),
                pltpu.SemaphoreType.DMA((2, chunks)),
            ],
            compiler_params=pltpu.CompilerParams(
                collective_id=0, has_side_effects=True, vmem_limit_bytes=60 * 1024 * 1024),
            name="sweep_ring",
        )(ratings_a, mask_a, users_a.T, items_a.T, ratings_b, mask_b, users_b.T, items_b.T)
        outs = pl.pallas_call(
            place,
            out_shape=(ut, vt, ut, vt),
            in_specs=[vmem] * 4,
            out_specs=[pl.BlockSpec(memory_space=pl.ANY)] * 4,
            scratch_shapes=[pltpu.SemaphoreType.DMA((4,))],
            compiler_params=pltpu.CompilerParams(vmem_limit_bytes=60 * 1024 * 1024),
            name="place",
        )(*outs)
        return tuple(o.T for o in outs)

    return jax.shard_map(device_body, mesh=mesh, in_specs=(row_spec,) * 8, out_specs=(row_spec,) * 4, check_vma=False)
```

```python
import functools
import math
import jax
import jax.numpy as jnp
from jax import lax
from jax.experimental import pallas as pl
from jax.experimental.pallas import tpu as pltpu
from jax.sharding import PartitionSpec as P

SWEEP_STEPS = 4
EPOCHS = 2
WEIGHT_DECAY = 0.05
CHUNK = 256
AHEAD = 3
STAGGER = 1400
MESH = pl.DeviceIdType.MESH


def sweep(u_ref, v_ref, rate_ref, flag_ref, step_u, step_v):
    chunks = range(v_ref.shape[0])
    f32, bf16 = jnp.float32, jnp.bfloat16
    user = u_ref[...]
    user_low = user.astype(bf16)
    user_low_t = user.T.astype(bf16)
    item_low = [v_ref[c].astype(bf16) for c in chunks]
    approx = [jnp.dot(user_low, item_low[c], preferred_element_type=f32) for c in chunks]
    err_low = []
    for c in chunks:
        cols = pl.ds(c * CHUNK, CHUNK)
        err_low.append((approx[c] - rate_ref[:, cols]).astype(bf16) * flag_ref[:, cols])
    part = [lax.dot_general(err_low[c], item_low[c], (((1,), (1,)), ((), ())), preferred_element_type=f32) for c in chunks]
    grad_v = [jnp.dot(user_low_t, err_low[c], preferred_element_type=f32) for c in chunks]
    for c in chunks:
        item = v_ref[c]
        v_ref[c] = item - step_v * (grad_v[c] + WEIGHT_DECAY * item)
    grad_u = (part[0] + part[1]) + (part[2] + part[3])
    u_ref[...] = user - step_u * (grad_u + WEIGHT_DECAY * user)


def kernel(shards, step_u, step_v, ra, ma, ua, va, rb, mb, ub, vb, ua_o, va_o, ub_o, vb_o,
           rates, masks, flags, items, last_items, users, users_in, users_out,
           load_sem, push_sem, send_sem, recv_sem, last_sem, user_sem, out_sem):
    me = lax.axis_index("shard")
    core = lax.rem(me, 2)
    base = me - core
    market = lax.rem(core + base // 2, 2)
    peer = base + 1 - core
    block = rates.shape[-1]
    chunks = block // CHUNK
    stages = EPOCHS * shards

    def dev(index):
        return {"shard": lax.rem(index + shards, shards)}

    def own(m):
        return (ra, ma, ua, va) if m == 0 else (rb, mb, ub, vb)

    def span(j):
        return pl.ds(pl.multiple_of(j * block, block), block)

    def pieces(m, q):
        j = lax.rem(base + core + q, shards)
        out = []
        for kind, buf in ((0, rates), (1, masks)):
            out.append(pltpu.make_async_copy(own(m)[kind].at[:, span(j)], buf.at[core, j], load_sem.at[kind, core, j]))
            out.append(pltpu.make_async_remote_copy(
                src_ref=own(1 - m)[kind].at[:, span(j)], dst_ref=buf.at[core, j], send_sem=push_sem.at[kind, j],
                recv_sem=load_sem.at[kind, core, j], device_id=dev(peer), device_id_type=MESH))
        return out

    def firsts(m):
        out = []
        for c in range(chunks):
            cols = pl.ds(c * CHUNK, CHUNK)
            out.append((pltpu.make_async_copy(own(m)[3].at[:, cols], items.at[core, c], recv_sem.at[core]),
                        pltpu.make_async_remote_copy(
                            src_ref=own(1 - m)[3].at[:, cols], dst_ref=items.at[core, c], send_sem=last_sem.at[2],
                            recv_sem=recv_sem.at[core], device_id=dev(peer), device_id_type=MESH)))
        return out

    def user_push(m):
        return pltpu.make_async_remote_copy(
            src_ref=own(1 - m)[2], dst_ref=users_in, send_sem=user_sem.at[0], recv_sem=user_sem.at[1],
            device_id=dev(peer), device_id_type=MESH)

    def hop(s):
        return pltpu.make_async_remote_copy(
            src_ref=items.at[s], dst_ref=items.at[s + 2], send_sem=send_sem.at[s],
            recv_sem=recv_sem.at[s + 2], device_id=dev(base - 1 - core), device_id_type=MESH)

    def home(s, target):
        return pltpu.make_async_remote_copy(
            src_ref=items.at[s], dst_ref=last_items.at[market], send_sem=send_sem.at[s],
            recv_sem=last_sem.at[market], device_id=dev(target), device_id_type=MESH)

    def user_home():
        return pltpu.make_async_remote_copy(
            src_ref=users.at[1 - core], dst_ref=users_out, send_sem=user_sem.at[2], recv_sem=user_sem.at[3],
            device_id=dev(peer), device_id_type=MESH)

    def landed(s):
        return pltpu.make_async_copy(items.at[s], items.at[s], recv_sem.at[s])

    barrier = pltpu.get_barrier_semaphore()
    for other in (base - 2, base - 1, peer, base + 2, base + 3):
        pl.semaphore_signal(barrier, inc=1, device_id=dev(other), device_id_type=MESH)

    for m in range(2):
        @pl.when(market == m)
        def _():
            for here, there in firsts(m):
                here.start()
            for q in range(AHEAD):
                for cp in pieces(m, q)[0::2]:
                    cp.start()
            users[core] = own(m)[2][...].T

    pl.semaphore_wait(barrier, 5)

    for m in range(2):
        @pl.when(market == m)
        def _():
            user_push(m).start()
            for here, there in firsts(m):
                there.start()
            for q in range(AHEAD):
                for cp in pieces(m, q)[1::2]:
                    cp.start()

    user_push(0).wait_recv()
    users[1 - core] = users_in[...].T

    def ready(role, j):
        for kind, buf in ((0, rates), (1, masks)):
            pltpu.make_async_copy(buf.at[role, j], buf.at[role, j], load_sem.at[kind, role, j]).wait()

    def visit(role, s, j):
        @pl.loop(0, SWEEP_STEPS)
        def _(n):
            sweep(users.at[role], items.at[s], rates.at[role, j], flags.at[role], step_u, step_v)

    @pl.when(market == 1)
    def _():
        pl.delay(STAGGER)

    @pl.loop(0, stages + 1)
    def _(s):
        j = lax.rem(base + s, shards)

        for m in range(2):
            @pl.when(jnp.logical_and(market == m, s + AHEAD < shards))
            def _():
                for cp in pieces(m, s + AHEAD):
                    cp.start()

        @pl.when(s < shards)
        def _():
            ready(0, j)

        @pl.when(jnp.logical_and(s >= 1, s <= shards))
        def _():
            ready(1, j)

        flags[0] = masks[0, j].astype(jnp.float32).astype(jnp.bfloat16)

        @pl.when(s > 0)
        def _():
            flags[1] = masks[1, j].astype(jnp.float32).astype(jnp.bfloat16)

        landed(s).wait()

        @pl.when(s > 0)
        def _():
            visit(1, s, j)

        @pl.when(s < stages)
        def _():
            visit(0, s, j)

        @pl.when(s < stages - 1)
        def _():
            hop(s).start()

        @pl.when(s == stages - 1)
        def _():
            home(s, base - 1).start()

    user_home().start()
    for m in range(2):
        @pl.when(market == m)
        def _():
            (ua_o, ub_o)[m][...] = users[core].T

    @pl.when(core == 1)
    def _():
        home(stages, base).start()

    def outs(src, m):
        return [pltpu.make_async_copy(src.at[c], (va_o, vb_o)[m].at[:, pl.ds(c * CHUNK, CHUNK)], out_sem.at[m, c])
                for c in range(chunks)]

    for m in range(2):
        mine = jnp.logical_and(core == 0, market == m)

        @pl.when(mine)
        def _():
            for cp in outs(items.at[stages], m):
                cp.start()

        @pl.when(jnp.logical_not(mine))
        def _():
            pltpu.make_async_copy(last_items.at[m], last_items.at[m], last_sem.at[m]).wait()
            for cp in outs(last_items.at[m], m):
                cp.start()

    user_home().wait()
    for m in range(2):
        @pl.when(market == m)
        def _():
            (ua_o, ub_o)[1 - m][...] = users_out[...].T
    for m in range(2):
        for cp in outs(last_items.at[m], m):
            cp.wait()
    user_push(0).wait_send()
    pltpu.make_async_copy(items.at[core], items.at[core], last_sem.at[2]).wait()

    @pl.loop(0, shards)
    def _(j):
        for kind, buf in ((0, rates), (1, masks)):
            pltpu.make_async_copy(buf.at[core, j], buf.at[core, j], push_sem.at[kind, j]).wait()

    @pl.loop(0, stages)
    def _(s):
        pltpu.make_async_copy(items.at[s], items.at[s], send_sem.at[s]).wait()

    @pl.when(core == 1)
    def _():
        home(stages, base).wait_send()


def place(ua, va, ub, vb, ua_o, va_o, ub_o, vb_o, sem):
    copies = [pltpu.make_async_copy(src, dst, sem.at[i])
              for i, (src, dst) in enumerate(((ua, ua_o), (va, va_o), (ub, ub_o), (vb, vb_o)))]
    for cp in copies:
        cp.start()
    for cp in copies:
        cp.wait()


def solution(mesh):
    shards = mesh.shape["shard"]
    row_spec = P(("rep", "shard"), None)

    def device_body(ratings_a, mask_a, users_a, items_a, ratings_b, mask_b, users_b, items_b):
        users_dev, rank = users_a.shape
        block = items_a.shape[0]
        chunks = block // CHUNK
        stages = EPOCHS * shards
        step_u = 0.5 * math.sqrt(rank) / (block + 2 * rank)
        step_v = 0.5 * math.sqrt(rank) / (users_dev + 2 * rank)
        hbm = pl.BlockSpec(memory_space=pltpu.HBM)
        vmem = pl.BlockSpec(memory_space=pltpu.VMEM)
        f32 = jnp.float32
        ut = jax.ShapeDtypeStruct((rank, users_dev), f32)
        vt = jax.ShapeDtypeStruct((rank, block), f32)
        outs = pl.pallas_call(
            functools.partial(kernel, shards, step_u, step_v),
            out_shape=(ut, vt, ut, vt),
            in_specs=[hbm, hbm, vmem, hbm] * 2,
            out_specs=[vmem] * 4,
            scratch_shapes=[
                pltpu.VMEM((2, shards, users_dev, block), f32),
                pltpu.VMEM((2, shards, users_dev, block), jnp.int32),
                pltpu.VMEM((2, users_dev, block), jnp.bfloat16),
                pltpu.VMEM((stages + 1, chunks, rank, CHUNK), f32),
                pltpu.VMEM((2, chunks, rank, CHUNK), f32),
                pltpu.VMEM((2, users_dev, rank), f32),
                pltpu.VMEM((rank, users_dev), f32),
                pltpu.VMEM((users_dev, rank), f32),
                pltpu.SemaphoreType.DMA((2, 2, shards)),
                pltpu.SemaphoreType.DMA((2, shards)),
                pltpu.SemaphoreType.DMA((stages + 1,)),
                pltpu.SemaphoreType.DMA((stages + 1,)),
                pltpu.SemaphoreType.DMA((3,)),
                pltpu.SemaphoreType.DMA((4,)),
                pltpu.SemaphoreType.DMA((2, chunks)),
            ],
            compiler_params=pltpu.CompilerParams(
                collective_id=0, has_side_effects=True, vmem_limit_bytes=60 * 1024 * 1024),
            name="sweep_ring",
        )(ratings_a, mask_a, users_a.T, items_a.T, ratings_b, mask_b, users_b.T, items_b.T)
        outs = pl.pallas_call(
            place,
            out_shape=(ut, vt, ut, vt),
            in_specs=[vmem] * 4,
            out_specs=[pl.BlockSpec(memory_space=pl.ANY)] * 4,
            scratch_shapes=[pltpu.SemaphoreType.DMA((4,))],
            compiler_params=pltpu.CompilerParams(vmem_limit_bytes=60 * 1024 * 1024),
            name="place",
        )(*outs)
        return tuple(o.T for o in outs)

    return jax.shard_map(device_body, mesh=mesh, in_specs=(row_spec,) * 8, out_specs=(row_spec,) * 4, check_vma=False)
```

```python
import functools
import math
import jax
import jax.numpy as jnp
from jax import lax
from jax.experimental import pallas as pl
from jax.experimental.pallas import tpu as pltpu
from jax.sharding import PartitionSpec as P

SWEEP_STEPS = 4
EPOCHS = 2
WEIGHT_DECAY = 0.05
CHUNK = 256
AHEAD = 3
STAGGER = 1400
MESH = pl.DeviceIdType.MESH


def sweep(u_ref, v_ref, rate_ref, flag_ref, step_u, step_v):
    chunks = range(v_ref.shape[0])
    f32, bf16 = jnp.float32, jnp.bfloat16
    user = u_ref[...]
    user_low = user.astype(bf16)
    user_low_t = user.T.astype(bf16)
    item_low = [v_ref[c].astype(bf16) for c in chunks]
    approx = [jnp.dot(user_low, item_low[c], preferred_element_type=f32) for c in chunks]
    err_low = []
    for c in chunks:
        cols = pl.ds(c * CHUNK, CHUNK)
        err_low.append((approx[c] - rate_ref[:, cols]).astype(bf16) * flag_ref[:, cols])
    part = [lax.dot_general(err_low[c], item_low[c], (((1,), (1,)), ((), ())), preferred_element_type=f32) for c in chunks]
    grad_v = [jnp.dot(user_low_t, err_low[c], preferred_element_type=f32) for c in chunks]
    for c in chunks:
        item = v_ref[c]
        v_ref[c] = item - step_v * (grad_v[c] + WEIGHT_DECAY * item)
    grad_u = (part[0] + part[1]) + (part[2] + part[3])
    u_ref[...] = user - step_u * (grad_u + WEIGHT_DECAY * user)


def kernel(shards, step_u, step_v, ra, ma, ua, va, rb, mb, ub, vb, ua_o, va_o, ub_o, vb_o,
           rates, masks, flags, items, last_items, users, users_in, users_out,
           load_sem, push_sem, send_sem, recv_sem, last_sem, user_sem, out_sem):
    me = lax.axis_index("shard")
    core = lax.rem(me, 2)
    base = me - core
    market = lax.rem(core + base // 2, 2)
    peer = base + 1 - core
    block = rates.shape[-1]
    chunks = block // CHUNK
    stages = EPOCHS * shards

    def dev(index):
        return {"shard": lax.rem(index + shards, shards)}

    def own(m):
        return (ra, ma, ua, va) if m == 0 else (rb, mb, ub, vb)

    def span(j):
        return pl.ds(pl.multiple_of(j * block, block), block)

    def pieces(m, q):
        j = lax.rem(base + core + q, shards)
        out = []
        for kind, buf in ((0, rates), (1, masks)):
            out.append(pltpu.make_async_copy(own(m)[kind].at[:, span(j)], buf.at[core, j], load_sem.at[kind, core, j]))
            out.append(pltpu.make_async_remote_copy(
                src_ref=own(1 - m)[kind].at[:, span(j)], dst_ref=buf.at[core, j], send_sem=push_sem.at[kind, j],
                recv_sem=load_sem.at[kind, core, j], device_id=dev(peer), device_id_type=MESH))
        return out

    def firsts(m):
        out = []
        for c in range(chunks):
            cols = pl.ds(c * CHUNK, CHUNK)
            out.append((pltpu.make_async_copy(own(m)[3].at[:, cols], items.at[core, c], recv_sem.at[core]),
                        pltpu.make_async_remote_copy(
                            src_ref=own(1 - m)[3].at[:, cols], dst_ref=items.at[core, c], send_sem=last_sem.at[2],
                            recv_sem=recv_sem.at[core], device_id=dev(peer), device_id_type=MESH)))
        return out

    def user_push(m):
        return pltpu.make_async_remote_copy(
            src_ref=own(1 - m)[2], dst_ref=users_in, send_sem=user_sem.at[0], recv_sem=user_sem.at[1],
            device_id=dev(peer), device_id_type=MESH)

    def hop(s):
        return pltpu.make_async_remote_copy(
            src_ref=items.at[s], dst_ref=items.at[s + 2], send_sem=send_sem.at[s],
            recv_sem=recv_sem.at[s + 2], device_id=dev(base - 1 - core), device_id_type=MESH)

    def home(s, target):
        return pltpu.make_async_remote_copy(
            src_ref=items.at[s], dst_ref=last_items.at[market], send_sem=send_sem.at[s],
            recv_sem=last_sem.at[market], device_id=dev(target), device_id_type=MESH)

    def user_home():
        return pltpu.make_async_remote_copy(
            src_ref=users.at[1 - core], dst_ref=users_out, send_sem=user_sem.at[2], recv_sem=user_sem.at[3],
            device_id=dev(peer), device_id_type=MESH)

    def landed(s):
        return pltpu.make_async_copy(items.at[s], items.at[s], recv_sem.at[s])

    barrier = pltpu.get_barrier_semaphore()
    for other in (base - 2, base - 1, peer, base + 2, base + 3):
        pl.semaphore_signal(barrier, inc=1, device_id=dev(other), device_id_type=MESH)

    for m in range(2):
        @pl.when(market == m)
        def _():
            for here, there in firsts(m):
                here.start()
            for q in range(AHEAD):
                for cp in pieces(m, q)[0::2]:
                    cp.start()
            users[core] = own(m)[2][...].T

    pl.semaphore_wait(barrier, 5)

    for m in range(2):
        @pl.when(market == m)
        def _():
            user_push(m).start()
            for here, there in firsts(m):
                there.start()
            for q in range(AHEAD):
                for cp in pieces(m, q)[1::2]:
                    cp.start()

    user_push(0).wait_recv()
    users[1 - core] = users_in[...].T

    def ready(role, j):
        for kind, buf in ((0, rates), (1, masks)):
            pltpu.make_async_copy(buf.at[role, j], buf.at[role, j], load_sem.at[kind, role, j]).wait()

    def visit(role, s, j):
        for _ in range(SWEEP_STEPS):
            sweep(users.at[role], items.at[s], rates.at[role, j], flags.at[role], step_u, step_v)

    @pl.loop(0, stages + 1)
    def _(s):
        j = lax.rem(base + s, shards)

        for m in range(2):
            @pl.when(jnp.logical_and(market == m, s + AHEAD < shards))
            def _():
                for cp in pieces(m, s + AHEAD):
                    cp.start()

        @pl.when(s < shards)
        def _():
            ready(0, j)

        @pl.when(jnp.logical_and(s >= 1, s <= shards))
        def _():
            ready(1, j)

        flags[0] = masks[0, j].astype(jnp.float32).astype(jnp.bfloat16)

        @pl.when(s > 0)
        def _():
            flags[1] = masks[1, j].astype(jnp.float32).astype(jnp.bfloat16)

        landed(s).wait()

        @pl.when(jnp.logical_and(s == 0, market == 1))
        def _():
            pl.delay(STAGGER)

        @pl.when(s > 0)
        def _():
            visit(1, s, j)

        @pl.when(s < stages)
        def _():
            visit(0, s, j)

        @pl.when(s < stages - 1)
        def _():
            hop(s).start()

        @pl.when(s == stages - 1)
        def _():
            home(s, base - 1).start()

    user_home().start()
    for m in range(2):
        @pl.when(market == m)
        def _():
            (ua_o, ub_o)[m][...] = users[core].T

    @pl.when(core == 1)
    def _():
        home(stages, base).start()

    def outs(src, m):
        return [pltpu.make_async_copy(src.at[c], (va_o, vb_o)[m].at[:, pl.ds(c * CHUNK, CHUNK)], out_sem.at[m, c])
                for c in range(chunks)]

    for m in range(2):
        mine = jnp.logical_and(core == 0, market == m)

        @pl.when(mine)
        def _():
            for cp in outs(items.at[stages], m):
                cp.start()

        @pl.when(jnp.logical_not(mine))
        def _():
            pltpu.make_async_copy(last_items.at[m], last_items.at[m], last_sem.at[m]).wait()
            for cp in outs(last_items.at[m], m):
                cp.start()

    user_home().wait()
    for m in range(2):
        @pl.when(market == m)
        def _():
            (ua_o, ub_o)[1 - m][...] = users_out[...].T
    for m in range(2):
        for cp in outs(last_items.at[m], m):
            cp.wait()
    user_push(0).wait_send()
    pltpu.make_async_copy(items.at[core], items.at[core], last_sem.at[2]).wait()

    @pl.loop(0, shards)
    def _(j):
        for kind, buf in ((0, rates), (1, masks)):
            pltpu.make_async_copy(buf.at[core, j], buf.at[core, j], push_sem.at[kind, j]).wait()

    @pl.loop(0, stages)
    def _(s):
        pltpu.make_async_copy(items.at[s], items.at[s], send_sem.at[s]).wait()

    @pl.when(core == 1)
    def _():
        home(stages, base).wait_send()


def place(ua, va, ub, vb, ua_o, va_o, ub_o, vb_o, sem):
    copies = [pltpu.make_async_copy(src, dst, sem.at[i])
              for i, (src, dst) in enumerate(((ua, ua_o), (va, va_o), (ub, ub_o), (vb, vb_o)))]
    for cp in copies:
        cp.start()
    for cp in copies:
        cp.wait()


def solution(mesh):
    shards = mesh.shape["shard"]
    row_spec = P(("rep", "shard"), None)

    def device_body(ratings_a, mask_a, users_a, items_a, ratings_b, mask_b, users_b, items_b):
        users_dev, rank = users_a.shape
        block = items_a.shape[0]
        chunks = block // CHUNK
        stages = EPOCHS * shards
        step_u = 0.5 * math.sqrt(rank) / (block + 2 * rank)
        step_v = 0.5 * math.sqrt(rank) / (users_dev + 2 * rank)
        hbm = pl.BlockSpec(memory_space=pltpu.HBM)
        vmem = pl.BlockSpec(memory_space=pltpu.VMEM)
        f32 = jnp.float32
        ut = jax.ShapeDtypeStruct((rank, users_dev), f32)
        vt = jax.ShapeDtypeStruct((rank, block), f32)
        outs = pl.pallas_call(
            functools.partial(kernel, shards, step_u, step_v),
            out_shape=(ut, vt, ut, vt),
            in_specs=[hbm, hbm, vmem, hbm] * 2,
            out_specs=[vmem] * 4,
            scratch_shapes=[
                pltpu.VMEM((2, shards, users_dev, block), f32),
                pltpu.VMEM((2, shards, users_dev, block), jnp.int32),
                pltpu.VMEM((2, users_dev, block), jnp.bfloat16),
                pltpu.VMEM((stages + 1, chunks, rank, CHUNK), f32),
                pltpu.VMEM((2, chunks, rank, CHUNK), f32),
                pltpu.VMEM((2, users_dev, rank), f32),
                pltpu.VMEM((rank, users_dev), f32),
                pltpu.VMEM((users_dev, rank), f32),
                pltpu.SemaphoreType.DMA((2, 2, shards)),
                pltpu.SemaphoreType.DMA((2, shards)),
                pltpu.SemaphoreType.DMA((stages + 1,)),
                pltpu.SemaphoreType.DMA((stages + 1,)),
                pltpu.SemaphoreType.DMA((3,)),
                pltpu.SemaphoreType.DMA((4,)),
                pltpu.SemaphoreType.DMA((2, chunks)),
            ],
            compiler_params=pltpu.CompilerParams(
                collective_id=0, has_side_effects=True, vmem_limit_bytes=60 * 1024 * 1024),
            name="sweep_ring",
        )(ratings_a, mask_a, users_a.T, items_a.T, ratings_b, mask_b, users_b.T, items_b.T)
        outs = pl.pallas_call(
            place,
            out_shape=(ut, vt, ut, vt),
            in_specs=[vmem] * 4,
            out_specs=[pl.BlockSpec(memory_space=pl.ANY)] * 4,
            scratch_shapes=[pltpu.SemaphoreType.DMA((4,))],
            compiler_params=pltpu.CompilerParams(vmem_limit_bytes=60 * 1024 * 1024),
            name="place",
        )(*outs)
        return tuple(o.T for o in outs)

    return jax.shard_map(device_body, mesh=mesh, in_specs=(row_spec,) * 8, out_specs=(row_spec,) * 4, check_vma=False)
```

```python
import functools
import math
import jax
import jax.numpy as jnp
from jax import lax
from jax.experimental import pallas as pl
from jax.experimental.pallas import tpu as pltpu
from jax.sharding import PartitionSpec as P

SWEEP_STEPS = 4
EPOCHS = 2
WEIGHT_DECAY = 0.05
CHUNK = 256
AHEAD = 3
STAGGER = 1400
LINK = 750
MESH = pl.DeviceIdType.MESH


def sweep(u_ref, v_ref, rate_ref, flag_ref, step_u, step_v):
    chunks = range(v_ref.shape[0])
    f32, bf16 = jnp.float32, jnp.bfloat16
    user = u_ref[...]
    user_low = user.astype(bf16)
    user_low_t = user.T.astype(bf16)
    item_low = [v_ref[c].astype(bf16) for c in chunks]
    approx = [jnp.dot(user_low, item_low[c], preferred_element_type=f32) for c in chunks]
    err_low = []
    for c in chunks:
        cols = pl.ds(c * CHUNK, CHUNK)
        err_low.append((approx[c] - rate_ref[:, cols]).astype(bf16) * flag_ref[:, cols])
    part = [lax.dot_general(err_low[c], item_low[c], (((1,), (1,)), ((), ())), preferred_element_type=f32) for c in chunks]
    grad_v = [jnp.dot(user_low_t, err_low[c], preferred_element_type=f32) for c in chunks]
    for c in chunks:
        item = v_ref[c]
        v_ref[c] = item - step_v * (grad_v[c] + WEIGHT_DECAY * item)
    grad_u = (part[0] + part[1]) + (part[2] + part[3])
    u_ref[...] = user - step_u * (grad_u + WEIGHT_DECAY * user)


def kernel(shards, step_u, step_v, ra, ma, ua, va, rb, mb, ub, vb, ua_o, va_o, ub_o, vb_o,
           rates, masks, flags, items, last_items, users, users_in, users_out,
           load_sem, push_sem, send_sem, recv_sem, last_sem, user_sem, out_sem, go_sem):
    me = lax.axis_index("shard")
    core = lax.rem(me, 2)
    base = me - core
    market = lax.rem(core + base // 2, 2)
    peer = base + 1 - core
    block = rates.shape[-1]
    chunks = block // CHUNK
    stages = EPOCHS * shards

    def dev(index):
        return {"shard": lax.rem(index + shards, shards)}

    def own(m):
        return (ra, ma, ua, va) if m == 0 else (rb, mb, ub, vb)

    def span(j):
        return pl.ds(pl.multiple_of(j * block, block), block)

    def pieces(m, q):
        j = lax.rem(base + core + q, shards)
        out = []
        for kind, buf in ((0, rates), (1, masks)):
            out.append(pltpu.make_async_copy(own(m)[kind].at[:, span(j)], buf.at[core, j], load_sem.at[kind, core, j]))
            out.append(pltpu.make_async_remote_copy(
                src_ref=own(1 - m)[kind].at[:, span(j)], dst_ref=buf.at[core, j], send_sem=push_sem.at[kind, j],
                recv_sem=load_sem.at[kind, core, j], device_id=dev(peer), device_id_type=MESH))
        return out

    def firsts(m):
        out = []
        for c in range(chunks):
            cols = pl.ds(c * CHUNK, CHUNK)
            out.append((pltpu.make_async_copy(own(m)[3].at[:, cols], items.at[core, c], recv_sem.at[core]),
                        pltpu.make_async_remote_copy(
                            src_ref=own(1 - m)[3].at[:, cols], dst_ref=items.at[core, c], send_sem=last_sem.at[2],
                            recv_sem=recv_sem.at[core], device_id=dev(peer), device_id_type=MESH)))
        return out

    def user_push(m):
        return pltpu.make_async_remote_copy(
            src_ref=own(1 - m)[2], dst_ref=users_in, send_sem=user_sem.at[0], recv_sem=user_sem.at[1],
            device_id=dev(peer), device_id_type=MESH)

    def hop(s):
        return pltpu.make_async_remote_copy(
            src_ref=items.at[s], dst_ref=items.at[s + 2], send_sem=send_sem.at[s],
            recv_sem=recv_sem.at[s + 2], device_id=dev(base - 1 - core), device_id_type=MESH)

    def home(s, target):
        return pltpu.make_async_remote_copy(
            src_ref=items.at[s], dst_ref=last_items.at[market], send_sem=send_sem.at[s],
            recv_sem=last_sem.at[market], device_id=dev(target), device_id_type=MESH)

    def user_home():
        return pltpu.make_async_remote_copy(
            src_ref=users.at[1 - core], dst_ref=users_out, send_sem=user_sem.at[2], recv_sem=user_sem.at[3],
            device_id=dev(peer), device_id_type=MESH)

    def landed(s):
        return pltpu.make_async_copy(items.at[s], items.at[s], recv_sem.at[s])

    barrier = pltpu.get_barrier_semaphore()
    chip, chips = base // 2, shards // 2
    near = ((peer, chip >= 0), (base - 2, chip >= 1), (base - 1, chip >= 1), (base + 2, chip < chips - 1),
            (base + 3, chip < chips - 1), (me - 4, chip >= 2), (me + 4, chip < chips - 2))
    for other, there in near:
        @pl.when(there)
        def _():
            pl.semaphore_signal(barrier, inc=1, device_id=dev(other), device_id_type=MESH)

    for m in range(2):
        @pl.when(market == m)
        def _():
            for here, there in firsts(m):
                here.start()
            for q in range(AHEAD):
                for cp in pieces(m, q)[0::2]:
                    cp.start()
            users[core] = own(m)[2][...].T

    pl.semaphore_wait(barrier, sum(there.astype(jnp.int32) for _, there in near))

    for m in range(2):
        @pl.when(market == m)
        def _():
            user_push(m).start()
            for here, there in firsts(m):
                there.start()
            for q in range(AHEAD):
                for cp in pieces(m, q)[1::2]:
                    cp.start()

    user_push(0).wait_recv()
    users[1 - core] = users_in[...].T

    even = lax.rem(chip, 2) == 0

    @pl.when(chip < chips - 1)
    def _():
        pl.semaphore_wait(go_sem, 1)

    @pl.when(jnp.logical_not(even))
    def _():
        pl.semaphore_signal(go_sem, inc=1, device_id=dev(me - 2), device_id_type=MESH)

    @pl.when(jnp.logical_and(jnp.logical_not(even), chip >= 2))
    def _():
        pl.semaphore_signal(go_sem, inc=1, device_id=dev(me - 4), device_id_type=MESH)

    def hold():
        ahead = chip // 2 + lax.rem(chip, 2)
        for n in range(1, chips // 2 + 1):
            @pl.when(ahead == n)
            def _():
                pl.delay(n * LINK)

        @pl.when(market == 1)
        def _():
            pl.delay(STAGGER)

    hold()

    def ready(role, j):
        for kind, buf in ((0, rates), (1, masks)):
            pltpu.make_async_copy(buf.at[role, j], buf.at[role, j], load_sem.at[kind, role, j]).wait()

    def visit(role, s, j):
        for _ in range(SWEEP_STEPS):
            sweep(users.at[role], items.at[s], rates.at[role, j], flags.at[role], step_u, step_v)

    @pl.loop(0, stages + 1)
    def _(s):
        j = lax.rem(base + s, shards)

        for m in range(2):
            @pl.when(jnp.logical_and(market == m, s + AHEAD < shards))
            def _():
                for cp in pieces(m, s + AHEAD):
                    cp.start()

        @pl.when(s < shards)
        def _():
            ready(0, j)

        @pl.when(jnp.logical_and(s >= 1, s <= shards))
        def _():
            ready(1, j)

        flags[0] = masks[0, j].astype(jnp.float32).astype(jnp.bfloat16)

        @pl.when(s > 0)
        def _():
            flags[1] = masks[1, j].astype(jnp.float32).astype(jnp.bfloat16)

        landed(s).wait()

        @pl.when(s > 0)
        def _():
            visit(1, s, j)

        @pl.when(s < stages)
        def _():
            visit(0, s, j)

        @pl.when(s < stages - 1)
        def _():
            hop(s).start()

        @pl.when(s == stages - 1)
        def _():
            home(s, base - 1).start()

    user_home().start()
    for m in range(2):
        @pl.when(market == m)
        def _():
            (ua_o, ub_o)[m][...] = users[core].T

    @pl.when(core == 1)
    def _():
        home(stages, base).start()

    def outs(src, m):
        return [pltpu.make_async_copy(src.at[c], (va_o, vb_o)[m].at[:, pl.ds(c * CHUNK, CHUNK)], out_sem.at[m, c])
                for c in range(chunks)]

    for m in range(2):
        mine = jnp.logical_and(core == 0, market == m)

        @pl.when(mine)
        def _():
            for cp in outs(items.at[stages], m):
                cp.start()

        @pl.when(jnp.logical_not(mine))
        def _():
            pltpu.make_async_copy(last_items.at[m], last_items.at[m], last_sem.at[m]).wait()
            for cp in outs(last_items.at[m], m):
                cp.start()

    user_home().wait()
    for m in range(2):
        @pl.when(market == m)
        def _():
            (ua_o, ub_o)[1 - m][...] = users_out[...].T
    for m in range(2):
        for cp in outs(last_items.at[m], m):
            cp.wait()
    user_push(0).wait_send()
    pltpu.make_async_copy(items.at[core], items.at[core], last_sem.at[2]).wait()

    @pl.loop(0, shards)
    def _(j):
        for kind, buf in ((0, rates), (1, masks)):
            pltpu.make_async_copy(buf.at[core, j], buf.at[core, j], push_sem.at[kind, j]).wait()

    @pl.loop(0, stages)
    def _(s):
        pltpu.make_async_copy(items.at[s], items.at[s], send_sem.at[s]).wait()

    @pl.when(core == 1)
    def _():
        home(stages, base).wait_send()


def place(ua, va, ub, vb, ua_o, va_o, ub_o, vb_o, sem):
    copies = [pltpu.make_async_copy(src, dst, sem.at[i])
              for i, (src, dst) in enumerate(((ua, ua_o), (va, va_o), (ub, ub_o), (vb, vb_o)))]
    for cp in copies:
        cp.start()
    for cp in copies:
        cp.wait()


def solution(mesh):
    shards = mesh.shape["shard"]
    row_spec = P(("rep", "shard"), None)

    def device_body(ratings_a, mask_a, users_a, items_a, ratings_b, mask_b, users_b, items_b):
        users_dev, rank = users_a.shape
        block = items_a.shape[0]
        chunks = block // CHUNK
        stages = EPOCHS * shards
        step_u = 0.5 * math.sqrt(rank) / (block + 2 * rank)
        step_v = 0.5 * math.sqrt(rank) / (users_dev + 2 * rank)
        hbm = pl.BlockSpec(memory_space=pltpu.HBM)
        vmem = pl.BlockSpec(memory_space=pltpu.VMEM)
        f32 = jnp.float32
        ut = jax.ShapeDtypeStruct((rank, users_dev), f32)
        vt = jax.ShapeDtypeStruct((rank, block), f32)
        outs = pl.pallas_call(
            functools.partial(kernel, shards, step_u, step_v),
            out_shape=(ut, vt, ut, vt),
            in_specs=[hbm, hbm, vmem, hbm] * 2,
            out_specs=[vmem] * 4,
            scratch_shapes=[
                pltpu.VMEM((2, shards, users_dev, block), f32),
                pltpu.VMEM((2, shards, users_dev, block), jnp.int32),
                pltpu.VMEM((2, users_dev, block), jnp.bfloat16),
                pltpu.VMEM((stages + 1, chunks, rank, CHUNK), f32),
                pltpu.VMEM((2, chunks, rank, CHUNK), f32),
                pltpu.VMEM((2, users_dev, rank), f32),
                pltpu.VMEM((rank, users_dev), f32),
                pltpu.VMEM((users_dev, rank), f32),
                pltpu.SemaphoreType.DMA((2, 2, shards)),
                pltpu.SemaphoreType.DMA((2, shards)),
                pltpu.SemaphoreType.DMA((stages + 1,)),
                pltpu.SemaphoreType.DMA((stages + 1,)),
                pltpu.SemaphoreType.DMA((3,)),
                pltpu.SemaphoreType.DMA((4,)),
                pltpu.SemaphoreType.DMA((2, chunks)),
                pltpu.SemaphoreType.REGULAR,
            ],
            compiler_params=pltpu.CompilerParams(
                collective_id=0, has_side_effects=True, vmem_limit_bytes=60 * 1024 * 1024),
            name="sweep_ring",
        )(ratings_a, mask_a, users_a.T, items_a.T, ratings_b, mask_b, users_b.T, items_b.T)
        outs = pl.pallas_call(
            place,
            out_shape=(ut, vt, ut, vt),
            in_specs=[vmem] * 4,
            out_specs=[pl.BlockSpec(memory_space=pl.ANY)] * 4,
            scratch_shapes=[pltpu.SemaphoreType.DMA((4,))],
            compiler_params=pltpu.CompilerParams(vmem_limit_bytes=60 * 1024 * 1024),
            name="place",
        )(*outs)
        return tuple(o.T for o in outs)

    return jax.shard_map(device_body, mesh=mesh, in_specs=(row_spec,) * 8, out_specs=(row_spec,) * 4, check_vma=False)
```

```python
import functools
import math
import jax
import jax.numpy as jnp
from jax import lax
from jax.experimental import pallas as pl
from jax.experimental.pallas import tpu as pltpu
from jax.sharding import PartitionSpec as P

SWEEP_STEPS = 4
EPOCHS = 2
WEIGHT_DECAY = 0.05
CHUNK = 256
AHEAD = 3
MESH = pl.DeviceIdType.MESH


def sweep(u_ref, v_ref, rate_ref, flag_ref, step_u, step_v):
    chunks = range(v_ref.shape[0])
    f32, bf16 = jnp.float32, jnp.bfloat16
    user = u_ref[...]
    user_low = user.astype(bf16)
    user_low_t = user.T.astype(bf16)
    item_low = [v_ref[c].astype(bf16) for c in chunks]
    approx = [jnp.dot(user_low, item_low[c], preferred_element_type=f32) for c in chunks]
    err_low = []
    for c in chunks:
        cols = pl.ds(c * CHUNK, CHUNK)
        err_low.append((approx[c] - rate_ref[:, cols]).astype(bf16) * flag_ref[:, cols])
    part = [lax.dot_general(err_low[c], item_low[c], (((1,), (1,)), ((), ())), preferred_element_type=f32) for c in chunks]
    grad_v = [jnp.dot(user_low_t, err_low[c], preferred_element_type=f32) for c in chunks]
    for c in chunks:
        item = v_ref[c]
        v_ref[c] = item - step_v * (grad_v[c] + WEIGHT_DECAY * item)
    grad_u = (part[0] + part[1]) + (part[2] + part[3])
    u_ref[...] = user - step_u * (grad_u + WEIGHT_DECAY * user)


def kernel(shards, step_u, step_v, ra, ma, ua, va, rb, mb, ub, vb, ua_o, va_o, ub_o, vb_o,
           rates, masks, flags, items, last_items, users, users_in, users_out,
           load_sem, push_sem, send_sem, recv_sem, last_sem, user_sem, out_sem, go_sem):
    me = lax.axis_index("shard")
    core = lax.rem(me, 2)
    base = me - core
    market = lax.rem(core + base // 2, 2)
    peer = base + 1 - core
    block = rates.shape[-1]
    chunks = block // CHUNK
    stages = EPOCHS * shards

    def dev(index):
        return {"shard": lax.rem(index + shards, shards)}

    def own(m):
        return (ra, ma, ua, va) if m == 0 else (rb, mb, ub, vb)

    def span(j):
        return pl.ds(pl.multiple_of(j * block, block), block)

    def pieces(m, q):
        j = lax.rem(base + core + q, shards)
        out = []
        for kind, buf in ((0, rates), (1, masks)):
            out.append(pltpu.make_async_copy(own(m)[kind].at[:, span(j)], buf.at[core, j], load_sem.at[kind, core, j]))
            out.append(pltpu.make_async_remote_copy(
                src_ref=own(1 - m)[kind].at[:, span(j)], dst_ref=buf.at[core, j], send_sem=push_sem.at[kind, j],
                recv_sem=load_sem.at[kind, core, j], device_id=dev(peer), device_id_type=MESH))
        return out

    def firsts(m):
        out = []
        for c in range(chunks):
            cols = pl.ds(c * CHUNK, CHUNK)
            out.append((pltpu.make_async_copy(own(m)[3].at[:, cols], items.at[core, c], recv_sem.at[core]),
                        pltpu.make_async_remote_copy(
                            src_ref=own(1 - m)[3].at[:, cols], dst_ref=items.at[core, c], send_sem=last_sem.at[2],
                            recv_sem=recv_sem.at[core], device_id=dev(peer), device_id_type=MESH)))
        return out

    def user_push(m):
        return pltpu.make_async_remote_copy(
            src_ref=own(1 - m)[2], dst_ref=users_in, send_sem=user_sem.at[0], recv_sem=user_sem.at[1],
            device_id=dev(peer), device_id_type=MESH)

    def hop(s):
        return pltpu.make_async_remote_copy(
            src_ref=items.at[s], dst_ref=items.at[s + 2], send_sem=send_sem.at[s],
            recv_sem=recv_sem.at[s + 2], device_id=dev(base - 1 - core), device_id_type=MESH)

    def home(s, target):
        return pltpu.make_async_remote_copy(
            src_ref=items.at[s], dst_ref=last_items.at[market], send_sem=send_sem.at[s],
            recv_sem=last_sem.at[market], device_id=dev(target), device_id_type=MESH)

    def user_home():
        return pltpu.make_async_remote_copy(
            src_ref=users.at[1 - core], dst_ref=users_out, send_sem=user_sem.at[2], recv_sem=user_sem.at[3],
            device_id=dev(peer), device_id_type=MESH)

    def landed(s):
        return pltpu.make_async_copy(items.at[s], items.at[s], recv_sem.at[s])

    barrier = pltpu.get_barrier_semaphore()
    chip, chips = base // 2, shards // 2
    near = ((peer, chip >= 0), (base - 2, chip >= 1), (base - 1, chip >= 1), (base + 2, chip < chips - 1),
            (base + 3, chip < chips - 1), (me - 4, chip >= 2), (me + 4, chip < chips - 2))
    for other, there in near:
        @pl.when(there)
        def _():
            pl.semaphore_signal(barrier, inc=1, device_id=dev(other), device_id_type=MESH)

    for m in range(2):
        @pl.when(market == m)
        def _():
            for here, there in firsts(m):
                here.start()
            for q in range(AHEAD):
                for cp in pieces(m, q)[0::2]:
                    cp.start()
            users[core] = own(m)[2][...].T

    pl.semaphore_wait(barrier, sum(there.astype(jnp.int32) for _, there in near))

    for m in range(2):
        @pl.when(market == m)
        def _():
            user_push(m).start()
            for here, there in firsts(m):
                there.start()
            for q in range(AHEAD):
                for cp in pieces(m, q)[1::2]:
                    cp.start()

    user_push(0).wait_recv()
    users[1 - core] = users_in[...].T

    even = lax.rem(chip, 2) == 0

    hears = jnp.logical_or(chip == 0, jnp.logical_and(jnp.logical_not(even), chip < chips - 1))

    @pl.when(hears)
    def _():
        pl.semaphore_wait(go_sem, 1)

    @pl.when(chip == 1)
    def _():
        pl.semaphore_signal(go_sem, inc=1, device_id=dev(me - 2), device_id_type=MESH)

    @pl.when(jnp.logical_and(jnp.logical_not(even), chip >= 2))
    def _():
        pl.semaphore_signal(go_sem, inc=1, device_id=dev(me - 4), device_id_type=MESH)

    def ready(role, j):
        for kind, buf in ((0, rates), (1, masks)):
            pltpu.make_async_copy(buf.at[role, j], buf.at[role, j], load_sem.at[kind, role, j]).wait()

    def visit(role, s, j):
        for _ in range(SWEEP_STEPS):
            sweep(users.at[role], items.at[s], rates.at[role, j], flags.at[role], step_u, step_v)

    @pl.loop(0, stages + 1)
    def _(s):
        j = lax.rem(base + s, shards)

        for m in range(2):
            @pl.when(jnp.logical_and(market == m, s + AHEAD < shards))
            def _():
                for cp in pieces(m, s + AHEAD):
                    cp.start()

        @pl.when(s < shards)
        def _():
            ready(0, j)

        @pl.when(jnp.logical_and(s >= 1, s <= shards))
        def _():
            ready(1, j)

        flags[0] = masks[0, j].astype(jnp.float32).astype(jnp.bfloat16)

        @pl.when(s > 0)
        def _():
            flags[1] = masks[1, j].astype(jnp.float32).astype(jnp.bfloat16)

        landed(s).wait()

        @pl.when(s > 0)
        def _():
            visit(1, s, j)

        @pl.when(s < stages)
        def _():
            visit(0, s, j)

        @pl.when(s < stages - 1)
        def _():
            hop(s).start()

        @pl.when(s == stages - 1)
        def _():
            home(s, base - 1).start()

    user_home().start()
    for m in range(2):
        @pl.when(market == m)
        def _():
            (ua_o, ub_o)[m][...] = users[core].T

    @pl.when(core == 1)
    def _():
        home(stages, base).start()

    def outs(src, m):
        return [pltpu.make_async_copy(src.at[c], (va_o, vb_o)[m].at[:, pl.ds(c * CHUNK, CHUNK)], out_sem.at[m, c])
                for c in range(chunks)]

    for m in range(2):
        mine = jnp.logical_and(core == 0, market == m)

        @pl.when(mine)
        def _():
            for cp in outs(items.at[stages], m):
                cp.start()

        @pl.when(jnp.logical_not(mine))
        def _():
            pltpu.make_async_copy(last_items.at[m], last_items.at[m], last_sem.at[m]).wait()
            for cp in outs(last_items.at[m], m):
                cp.start()

    user_home().wait()
    for m in range(2):
        @pl.when(market == m)
        def _():
            (ua_o, ub_o)[1 - m][...] = users_out[...].T
    for m in range(2):
        for cp in outs(last_items.at[m], m):
            cp.wait()
    user_push(0).wait_send()
    pltpu.make_async_copy(items.at[core], items.at[core], last_sem.at[2]).wait()

    @pl.loop(0, shards)
    def _(j):
        for kind, buf in ((0, rates), (1, masks)):
            pltpu.make_async_copy(buf.at[core, j], buf.at[core, j], push_sem.at[kind, j]).wait()

    @pl.loop(0, stages)
    def _(s):
        pltpu.make_async_copy(items.at[s], items.at[s], send_sem.at[s]).wait()

    @pl.when(core == 1)
    def _():
        home(stages, base).wait_send()


def place(ua, va, ub, vb, ua_o, va_o, ub_o, vb_o, sem):
    copies = [pltpu.make_async_copy(src, dst, sem.at[i])
              for i, (src, dst) in enumerate(((ua, ua_o), (va, va_o), (ub, ub_o), (vb, vb_o)))]
    for cp in copies:
        cp.start()
    for cp in copies:
        cp.wait()


def solution(mesh):
    shards = mesh.shape["shard"]
    row_spec = P(("rep", "shard"), None)

    def device_body(ratings_a, mask_a, users_a, items_a, ratings_b, mask_b, users_b, items_b):
        users_dev, rank = users_a.shape
        block = items_a.shape[0]
        chunks = block // CHUNK
        stages = EPOCHS * shards
        step_u = 0.5 * math.sqrt(rank) / (block + 2 * rank)
        step_v = 0.5 * math.sqrt(rank) / (users_dev + 2 * rank)
        hbm = pl.BlockSpec(memory_space=pltpu.HBM)
        vmem = pl.BlockSpec(memory_space=pltpu.VMEM)
        f32 = jnp.float32
        ut = jax.ShapeDtypeStruct((rank, users_dev), f32)
        vt = jax.ShapeDtypeStruct((rank, block), f32)
        outs = pl.pallas_call(
            functools.partial(kernel, shards, step_u, step_v),
            out_shape=(ut, vt, ut, vt),
            in_specs=[hbm, hbm, vmem, hbm] * 2,
            out_specs=[vmem] * 4,
            scratch_shapes=[
                pltpu.VMEM((2, shards, users_dev, block), f32),
                pltpu.VMEM((2, shards, users_dev, block), jnp.int32),
                pltpu.VMEM((2, users_dev, block), jnp.bfloat16),
                pltpu.VMEM((stages + 1, chunks, rank, CHUNK), f32),
                pltpu.VMEM((2, chunks, rank, CHUNK), f32),
                pltpu.VMEM((2, users_dev, rank), f32),
                pltpu.VMEM((rank, users_dev), f32),
                pltpu.VMEM((users_dev, rank), f32),
                pltpu.SemaphoreType.DMA((2, 2, shards)),
                pltpu.SemaphoreType.DMA((2, shards)),
                pltpu.SemaphoreType.DMA((stages + 1,)),
                pltpu.SemaphoreType.DMA((stages + 1,)),
                pltpu.SemaphoreType.DMA((3,)),
                pltpu.SemaphoreType.DMA((4,)),
                pltpu.SemaphoreType.DMA((2, chunks)),
                pltpu.SemaphoreType.REGULAR,
            ],
            compiler_params=pltpu.CompilerParams(
                collective_id=0, has_side_effects=True, vmem_limit_bytes=60 * 1024 * 1024),
            name="sweep_ring",
        )(ratings_a, mask_a, users_a.T, items_a.T, ratings_b, mask_b, users_b.T, items_b.T)
        outs = pl.pallas_call(
            place,
            out_shape=(ut, vt, ut, vt),
            in_specs=[vmem] * 4,
            out_specs=[pl.BlockSpec(memory_space=pl.ANY)] * 4,
            scratch_shapes=[pltpu.SemaphoreType.DMA((4,))],
            compiler_params=pltpu.CompilerParams(vmem_limit_bytes=60 * 1024 * 1024),
            name="place",
        )(*outs)
        return tuple(o.T for o in outs)

    return jax.shard_map(device_body, mesh=mesh, in_specs=(row_spec,) * 8, out_specs=(row_spec,) * 4, check_vma=False)
```

```python
import functools
import math
import jax
import jax.numpy as jnp
from jax import lax
from jax.experimental import pallas as pl
from jax.experimental.pallas import tpu as pltpu
from jax.sharding import PartitionSpec as P

SWEEP_STEPS = 4
EPOCHS = 2
WEIGHT_DECAY = 0.05
CHUNK = 256
MESH = pl.DeviceIdType.MESH


def sweep(u_ref, v_ref, rate_ref, flag_ref, step_u, step_v):
    chunks = range(v_ref.shape[0])
    f32, bf16 = jnp.float32, jnp.bfloat16
    user = u_ref[...]
    user_low = user.astype(bf16)
    user_low_t = user.T.astype(bf16)
    item_low = [v_ref[c].astype(bf16) for c in chunks]
    approx = [jnp.dot(user_low, item_low[c], preferred_element_type=f32) for c in chunks]
    err_low = []
    for c in chunks:
        cols = pl.ds(c * CHUNK, CHUNK)
        err_low.append((approx[c] - rate_ref[:, cols]).astype(bf16) * flag_ref[:, cols])
    part = [lax.dot_general(err_low[c], item_low[c], (((1,), (1,)), ((), ())), preferred_element_type=f32) for c in chunks]
    grad_v = [jnp.dot(user_low_t, err_low[c], preferred_element_type=f32) for c in chunks]
    for c in chunks:
        item = v_ref[c]
        v_ref[c] = item - step_v * (grad_v[c] + WEIGHT_DECAY * item)
    grad_u = (part[0] + part[1]) + (part[2] + part[3])
    u_ref[...] = user - step_u * (grad_u + WEIGHT_DECAY * user)


def kernel(shards, step_u, step_v, ra, ma, ua, va, rb, mb, ub, vb, ua_o, va_o, ub_o, vb_o,
           rates, masks, flags, items, users, load_sem, first_sem, send_sem, recv_sem, out_sem):
    me = lax.axis_index("shard")
    left = lax.rem(me + shards - 1, shards)
    right = lax.rem(me + 1, shards)
    block = rates.shape[-1]
    chunks = block // CHUNK
    stages = EPOCHS * shards
    rate_in, mask_in = (ra, rb), (ma, mb)

    def loads(m, t):
        j = lax.rem(me + t, shards)
        cols = pl.ds(pl.multiple_of(j * block, block), block)
        return (pltpu.make_async_copy(rate_in[m].at[:, cols], rates.at[m, j], load_sem.at[0, m, j]),
                pltpu.make_async_copy(mask_in[m].at[:, cols], masks.at[m, j], load_sem.at[1, m, j]))

    def first(m, c):
        return pltpu.make_async_copy((va, vb)[m].at[:, pl.ds(c * CHUNK, CHUNK)], items.at[m, 0, c], first_sem.at[m, c])

    def last(m, c):
        return pltpu.make_async_copy(items.at[m, stages, c], (va_o, vb_o)[m].at[:, pl.ds(c * CHUNK, CHUNK)], out_sem.at[m, c])

    def hop(m, t):
        return pltpu.make_async_remote_copy(
            src_ref=items.at[m, t], dst_ref=items.at[m, t + 1], send_sem=send_sem.at[m, t],
            recv_sem=recv_sem.at[m, t + 1], device_id={"shard": left}, device_id_type=MESH)

    for m in range(2):
        for c in range(chunks):
            first(m, c).start()
        for cp in loads(m, 0):
            cp.start()

    barrier = pltpu.get_barrier_semaphore()
    for other in (left, right):
        pl.semaphore_signal(barrier, inc=1, device_id={"shard": other}, device_id_type=MESH)

    @pl.loop(1, shards)
    def _(t):
        for m in range(2):
            for cp in loads(m, t):
                cp.start()

    users[0] = ua[...].T
    users[1] = ub[...].T
    for m in range(2):
        for c in range(chunks):
            first(m, c).wait()
    pl.semaphore_wait(barrier, 2)

    @pl.loop(0, stages)
    def _(t):
        j = lax.rem(me + t, shards)
        for m in range(2):
            @pl.when(t < shards)
            def _():
                for cp in loads(m, t):
                    cp.wait()
            flags[m] = masks[m, j].astype(jnp.float32).astype(jnp.bfloat16)
        for m in range(2):
            @pl.when(t > 0)
            def _():
                hop(m, t - 1).wait_recv()

            for _ in range(SWEEP_STEPS):
                sweep(users.at[m], items.at[m, t], rates.at[m, j], flags.at[m], step_u, step_v)
            hop(m, t).start()

    ua_o[...] = users[0].T
    ub_o[...] = users[1].T
    for m in range(2):
        hop(m, stages - 1).wait_recv()
        for c in range(chunks):
            last(m, c).start()
    for m in range(2):
        for c in range(chunks):
            last(m, c).wait()

    @pl.loop(0, stages)
    def _(t):
        for m in range(2):
            hop(m, t).wait_send()


def place(ua, va, ub, vb, ua_o, va_o, ub_o, vb_o, sem):
    copies = [pltpu.make_async_copy(src, dst, sem.at[i])
              for i, (src, dst) in enumerate(((ua, ua_o), (va, va_o), (ub, ub_o), (vb, vb_o)))]
    for cp in copies:
        cp.start()
    for cp in copies:
        cp.wait()


def solution(mesh):
    shards = mesh.shape["shard"]
    row_spec = P(("rep", "shard"), None)

    def device_body(ratings_a, mask_a, users_a, items_a, ratings_b, mask_b, users_b, items_b):
        users_dev, rank = users_a.shape
        block = items_a.shape[0]
        chunks = block // CHUNK
        stages = EPOCHS * shards
        step_u = 0.5 * math.sqrt(rank) / (block + 2 * rank)
        step_v = 0.5 * math.sqrt(rank) / (users_dev + 2 * rank)
        hbm = pl.BlockSpec(memory_space=pltpu.HBM)
        vmem = pl.BlockSpec(memory_space=pltpu.VMEM)
        f32 = jnp.float32
        ut = jax.ShapeDtypeStruct((rank, users_dev), f32)
        vt = jax.ShapeDtypeStruct((rank, block), f32)
        outs = pl.pallas_call(
            functools.partial(kernel, shards, step_u, step_v),
            out_shape=(ut, vt, ut, vt),
            in_specs=[hbm, hbm, vmem, hbm] * 2,
            out_specs=[vmem] * 4,
            scratch_shapes=[
                pltpu.VMEM((2, shards, users_dev, block), f32),
                pltpu.VMEM((2, shards, users_dev, block), jnp.int32),
                pltpu.VMEM((2, users_dev, block), jnp.bfloat16),
                pltpu.VMEM((2, stages + 1, chunks, rank, CHUNK), f32),
                pltpu.VMEM((2, users_dev, rank), f32),
                pltpu.SemaphoreType.DMA((2, 2, shards)),
                pltpu.SemaphoreType.DMA((2, chunks)),
                pltpu.SemaphoreType.DMA((2, stages)),
                pltpu.SemaphoreType.DMA((2, stages + 1)),
                pltpu.SemaphoreType.DMA((2, chunks)),
            ],
            compiler_params=pltpu.CompilerParams(
                collective_id=0, has_side_effects=True, vmem_limit_bytes=60 * 1024 * 1024),
            name="sweep_ring",
        )(ratings_a, mask_a, users_a.T, items_a.T, ratings_b, mask_b, users_b.T, items_b.T)
        outs = pl.pallas_call(
            place,
            out_shape=(ut, vt, ut, vt),
            in_specs=[vmem] * 4,
            out_specs=[pl.BlockSpec(memory_space=pl.ANY)] * 4,
            scratch_shapes=[pltpu.SemaphoreType.DMA((4,))],
            compiler_params=pltpu.CompilerParams(vmem_limit_bytes=60 * 1024 * 1024),
            name="place",
        )(*outs)
        return tuple(o.T for o in outs)

    return jax.shard_map(device_body, mesh=mesh, in_specs=(row_spec,) * 8, out_specs=(row_spec,) * 4, check_vma=False)
```

```python
import functools
import math
import jax
import jax.numpy as jnp
from jax import lax
from jax.experimental import pallas as pl
from jax.experimental.pallas import tpu as pltpu
from jax.sharding import PartitionSpec as P

SWEEP_STEPS = 4
EPOCHS = 2
WEIGHT_DECAY = 0.05
CHUNK = 256
MESH = pl.DeviceIdType.MESH


def sweep(u_ref, v_ref, rate_ref, flag_ref, step_u, step_v):
    chunks = range(v_ref.shape[0])
    f32, bf16 = jnp.float32, jnp.bfloat16
    user = u_ref[...]
    user_low = user.astype(bf16)
    user_low_t = user.T.astype(bf16)
    item_low = [v_ref[c].astype(bf16) for c in chunks]
    approx = [jnp.dot(user_low, item_low[c], preferred_element_type=f32) for c in chunks]
    err_low = []
    for c in chunks:
        cols = pl.ds(c * CHUNK, CHUNK)
        err_low.append((approx[c] - rate_ref[:, cols]).astype(bf16) * flag_ref[:, cols])
    part = [lax.dot_general(err_low[c], item_low[c], (((1,), (1,)), ((), ())), preferred_element_type=f32) for c in chunks]
    grad_v = [jnp.dot(user_low_t, err_low[c], preferred_element_type=f32) for c in chunks]
    for c in chunks:
        item = v_ref[c]
        v_ref[c] = item - step_v * (grad_v[c] + WEIGHT_DECAY * item)
    grad_u = (part[0] + part[1]) + (part[2] + part[3])
    u_ref[...] = user - step_u * (grad_u + WEIGHT_DECAY * user)


def kernel(shards, step_u, step_v, ra, ma, ua, va, rb, mb, ub, vb, ua_o, va_o, ub_o, vb_o,
           rates, masks, flags, items, users, users_t, load_sem, first_sem, send_sem, recv_sem, out_sem, user_sem):
    me = lax.axis_index("shard")
    left = lax.rem(me + shards - 1, shards)
    right = lax.rem(me + 1, shards)
    block = rates.shape[-1]
    chunks = block // CHUNK
    stages = EPOCHS * shards
    rate_in, mask_in = (ra, rb), (ma, mb)

    def loads(m, t):
        j = lax.rem(me + t, shards)
        cols = pl.ds(pl.multiple_of(j * block, block), block)
        return (pltpu.make_async_copy(rate_in[m].at[:, cols], rates.at[m, j], load_sem.at[0, m, j]),
                pltpu.make_async_copy(mask_in[m].at[:, cols], masks.at[m, j], load_sem.at[1, m, j]))

    def first(m, c):
        return pltpu.make_async_copy((va, vb)[m].at[:, pl.ds(c * CHUNK, CHUNK)], items.at[m, 0, c], first_sem.at[m, c])

    def last(m, c):
        return pltpu.make_async_copy(items.at[m, stages, c], (va_o, vb_o)[m].at[:, pl.ds(c * CHUNK, CHUNK)], out_sem.at[m, c])

    def hop(m, t):
        return pltpu.make_async_remote_copy(
            src_ref=items.at[m, t], dst_ref=items.at[m, t + 1], send_sem=send_sem.at[m, t],
            recv_sem=recv_sem.at[m, t + 1], device_id={"shard": left}, device_id_type=MESH)

    def user_in(m):
        return pltpu.make_async_copy((ua, ub)[m], users_t.at[m], user_sem.at[m])

    def user_out(m):
        return pltpu.make_async_copy(users_t.at[m], (ua_o, ub_o)[m], user_sem.at[m])

    for m in range(2):
        for c in range(chunks):
            first(m, c).start()
        user_in(m).start()
        for cp in loads(m, 0):
            cp.start()

    barrier = pltpu.get_barrier_semaphore()
    for other in (left, right):
        pl.semaphore_signal(barrier, inc=1, device_id={"shard": other}, device_id_type=MESH)

    @pl.loop(1, shards)
    def _(t):
        for m in range(2):
            for cp in loads(m, t):
                cp.start()

    for m in range(2):
        user_in(m).wait()
        users[m] = users_t[m].T
        for c in range(chunks):
            first(m, c).wait()

    @pl.loop(0, stages)
    def _(t):
        j = lax.rem(me + t, shards)
        for m in range(2):
            @pl.when(t < shards)
            def _():
                for cp in loads(m, t):
                    cp.wait()
            flags[m] = masks[m, j].astype(jnp.float32).astype(jnp.bfloat16)
        for m in range(2):
            @pl.when(t > 0)
            def _():
                hop(m, t - 1).wait_recv()

            for _ in range(SWEEP_STEPS):
                sweep(users.at[m], items.at[m, t], rates.at[m, j], flags.at[m], step_u, step_v)
            if m == 0:
                @pl.when(t == 0)
                def _():
                    pl.semaphore_wait(barrier, 2)
            hop(m, t).start()

    for m in range(2):
        users_t[m] = users[m].T
    for m in range(2):
        user_out(m).start()
        hop(m, stages - 1).wait_recv()
        for c in range(chunks):
            last(m, c).start()
    for m in range(2):
        for c in range(chunks):
            last(m, c).wait()
        user_out(m).wait()

    @pl.loop(0, stages)
    def _(t):
        for m in range(2):
            hop(m, t).wait_send()


def place(ua, va, ub, vb, ua_o, va_o, ub_o, vb_o, sem):
    copies = [pltpu.make_async_copy(src, dst, sem.at[i])
              for i, (src, dst) in enumerate(((ua, ua_o), (va, va_o), (ub, ub_o), (vb, vb_o)))]
    for cp in copies:
        cp.start()
    for cp in copies:
        cp.wait()


def solution(mesh):
    shards = mesh.shape["shard"]
    row_spec = P(("rep", "shard"), None)

    def device_body(ratings_a, mask_a, users_a, items_a, ratings_b, mask_b, users_b, items_b):
        users_dev, rank = users_a.shape
        block = items_a.shape[0]
        chunks = block // CHUNK
        stages = EPOCHS * shards
        step_u = 0.5 * math.sqrt(rank) / (block + 2 * rank)
        step_v = 0.5 * math.sqrt(rank) / (users_dev + 2 * rank)
        hbm = pl.BlockSpec(memory_space=pltpu.HBM)
        vmem = pl.BlockSpec(memory_space=pltpu.VMEM)
        f32 = jnp.float32
        ut = jax.ShapeDtypeStruct((rank, users_dev), f32)
        vt = jax.ShapeDtypeStruct((rank, block), f32)
        outs = pl.pallas_call(
            functools.partial(kernel, shards, step_u, step_v),
            out_shape=(ut, vt, ut, vt),
            in_specs=[hbm] * 8,
            out_specs=[hbm] * 4,
            scratch_shapes=[
                pltpu.VMEM((2, shards, users_dev, block), f32),
                pltpu.VMEM((2, shards, users_dev, block), jnp.int32),
                pltpu.VMEM((2, users_dev, block), jnp.bfloat16),
                pltpu.VMEM((2, stages + 1, chunks, rank, CHUNK), f32),
                pltpu.VMEM((2, users_dev, rank), f32),
                pltpu.VMEM((2, rank, users_dev), f32),
                pltpu.SemaphoreType.DMA((2, 2, shards)),
                pltpu.SemaphoreType.DMA((2, chunks)),
                pltpu.SemaphoreType.DMA((2, stages)),
                pltpu.SemaphoreType.DMA((2, stages + 1)),
                pltpu.SemaphoreType.DMA((2, chunks)),
                pltpu.SemaphoreType.DMA((2,)),
            ],
            compiler_params=pltpu.CompilerParams(
                collective_id=0, has_side_effects=True, vmem_limit_bytes=60 * 1024 * 1024),
            name="sweep_ring",
        )(ratings_a, mask_a, users_a.T, items_a.T, ratings_b, mask_b, users_b.T, items_b.T)
        outs = pl.pallas_call(
            place,
            out_shape=(ut, vt, ut, vt),
            in_specs=[vmem] * 4,
            out_specs=[pl.BlockSpec(memory_space=pl.ANY)] * 4,
            scratch_shapes=[pltpu.SemaphoreType.DMA((4,))],
            compiler_params=pltpu.CompilerParams(vmem_limit_bytes=60 * 1024 * 1024),
            name="place",
        )(*outs)
        return tuple(o.T for o in outs)

    return jax.shard_map(device_body, mesh=mesh, in_specs=(row_spec,) * 8, out_specs=(row_spec,) * 4, check_vma=False)
```

```python
import functools
import math
import jax
import jax.numpy as jnp
from jax import lax
from jax.experimental import pallas as pl
from jax.experimental.pallas import tpu as pltpu
from jax.sharding import PartitionSpec as P

SWEEP_STEPS = 4
EPOCHS = 2
WEIGHT_DECAY = 0.05
CHUNK = 256
AHEAD = 3
STAGGER = 1400
MESH = pl.DeviceIdType.MESH


def sweep(u_ref, v_ref, rate_ref, flag_ref, step_u, step_v):
    chunks = range(v_ref.shape[0])
    f32, bf16 = jnp.float32, jnp.bfloat16
    user = u_ref[...]
    user_low = user.astype(bf16)
    user_low_t = user.T.astype(bf16)
    item_low = [v_ref[c].astype(bf16) for c in chunks]
    approx = [jnp.dot(user_low, item_low[c], preferred_element_type=f32) for c in chunks]
    err_low = []
    for c in chunks:
        cols = pl.ds(c * CHUNK, CHUNK)
        err_low.append((approx[c] - rate_ref[:, cols]).astype(bf16) * flag_ref[:, cols])
    part = [lax.dot_general(err_low[c], item_low[c], (((1,), (1,)), ((), ())), preferred_element_type=f32) for c in chunks]
    grad_v = [jnp.dot(user_low_t, err_low[c], preferred_element_type=f32) for c in chunks]
    for c in chunks:
        item = v_ref[c]
        v_ref[c] = item - step_v * (grad_v[c] + WEIGHT_DECAY * item)
    grad_u = (part[0] + part[1]) + (part[2] + part[3])
    u_ref[...] = user - step_u * (grad_u + WEIGHT_DECAY * user)


def kernel(shards, step_u, step_v, ra, ma, ua, va, rb, mb, ub, vb, ua_o, va_o, ub_o, vb_o,
           rates, masks, flags, items, last_items, users, users_t, users_in, users_out,
           load_sem, push_sem, send_sem, recv_sem, last_sem, user_sem, out_sem, go_sem, pair_sem):
    me = lax.axis_index("shard")
    core = lax.rem(me, 2)
    base = me - core
    market = lax.rem(core + base // 2, 2)
    peer = base + 1 - core
    block = rates.shape[-1]
    chunks = block // CHUNK
    stages = EPOCHS * shards

    def dev(index):
        return {"shard": lax.rem(index + shards, shards)}

    def own(m):
        return (ra, ma, ua, va) if m == 0 else (rb, mb, ub, vb)

    def span(j):
        return pl.ds(pl.multiple_of(j * block, block), block)

    def pieces(m, q):
        j = lax.rem(base + core + q, shards)
        out = []
        for kind, buf in ((0, rates), (1, masks)):
            out.append(pltpu.make_async_copy(own(m)[kind].at[:, span(j)], buf.at[core, j], load_sem.at[kind, core, j]))
            out.append(pltpu.make_async_remote_copy(
                src_ref=own(1 - m)[kind].at[:, span(j)], dst_ref=buf.at[core, j], send_sem=push_sem.at[kind, j],
                recv_sem=load_sem.at[kind, core, j], device_id=dev(peer), device_id_type=MESH))
        return out

    def firsts(m):
        out = []
        for c in range(chunks):
            cols = pl.ds(c * CHUNK, CHUNK)
            out.append((pltpu.make_async_copy(own(m)[3].at[:, cols], items.at[core, c], recv_sem.at[core]),
                        pltpu.make_async_remote_copy(
                            src_ref=own(1 - m)[3].at[:, cols], dst_ref=items.at[core, c], send_sem=last_sem.at[2],
                            recv_sem=recv_sem.at[core], device_id=dev(peer), device_id_type=MESH)))
        return out

    def user_push(m):
        return pltpu.make_async_remote_copy(
            src_ref=own(1 - m)[2], dst_ref=users_in, send_sem=user_sem.at[0], recv_sem=user_sem.at[1],
            device_id=dev(peer), device_id_type=MESH)

    def hop(s):
        return pltpu.make_async_remote_copy(
            src_ref=items.at[s], dst_ref=items.at[s + 2], send_sem=send_sem.at[s],
            recv_sem=recv_sem.at[s + 2], device_id=dev(base - 1 - core), device_id_type=MESH)

    def home(s, target):
        return pltpu.make_async_remote_copy(
            src_ref=items.at[s], dst_ref=last_items.at[market], send_sem=send_sem.at[s],
            recv_sem=last_sem.at[market], device_id=dev(target), device_id_type=MESH)

    def user_home():
        return pltpu.make_async_remote_copy(
            src_ref=users.at[1 - core], dst_ref=users_out, send_sem=user_sem.at[2], recv_sem=user_sem.at[3],
            device_id=dev(peer), device_id_type=MESH)

    def landed(s):
        return pltpu.make_async_copy(items.at[s], items.at[s], recv_sem.at[s])

    barrier = pltpu.get_barrier_semaphore()
    chip, chips = base // 2, shards // 2
    near = ((peer, chip >= 0), (base - 2, chip >= 1), (base - 1, chip >= 1), (base + 2, chip < chips - 1),
            (base + 3, chip < chips - 1), (me - 4, chip >= 2), (me + 4, chip < chips - 2))
    for other, there in near:
        @pl.when(there)
        def _():
            pl.semaphore_signal(barrier, inc=1, device_id=dev(other), device_id_type=MESH)

    for m in range(2):
        @pl.when(market == m)
        def _():
            for here, there in firsts(m):
                here.start()
            for q in range(AHEAD):
                for cp in pieces(m, q)[0::2]:
                    cp.start()
            pltpu.make_async_copy(own(m)[2], users_t, user_sem.at[4]).start()

    pl.semaphore_wait(barrier, sum(there.astype(jnp.int32) for _, there in near))

    for m in range(2):
        @pl.when(market == m)
        def _():
            user_push(m).start()
            for here, there in firsts(m):
                there.start()
            for q in range(AHEAD):
                for cp in pieces(m, q)[1::2]:
                    cp.start()

    pltpu.make_async_copy(users_t, users_t, user_sem.at[4]).wait()
    users[core] = users_t[...].T
    user_push(0).wait_recv()
    users[1 - core] = users_in[...].T

    even = lax.rem(chip, 2) == 0

    hears = jnp.logical_or(chip == 0, jnp.logical_and(jnp.logical_not(even), chip < chips - 1))

    @pl.when(hears)
    def _():
        pl.semaphore_wait(go_sem, 1)

    @pl.when(chip == 1)
    def _():
        pl.semaphore_signal(go_sem, inc=1, device_id=dev(me - 2), device_id_type=MESH)

    @pl.when(jnp.logical_and(jnp.logical_not(even), chip >= 2))
    def _():
        pl.semaphore_signal(go_sem, inc=1, device_id=dev(me - 4), device_id_type=MESH)

    def ready(role, j):
        for kind, buf in ((0, rates), (1, masks)):
            pltpu.make_async_copy(buf.at[role, j], buf.at[role, j], load_sem.at[kind, role, j]).wait()

    def visit(role, s, j):
        for _ in range(SWEEP_STEPS):
            sweep(users.at[role], items.at[s], rates.at[role, j], flags.at[role], step_u, step_v)

    @pl.loop(0, stages + 1)
    def _(s):
        j = lax.rem(base + s, shards)

        for m in range(2):
            @pl.when(jnp.logical_and(market == m, s + AHEAD < shards))
            def _():
                for cp in pieces(m, s + AHEAD):
                    cp.start()

        @pl.when(s < shards)
        def _():
            ready(0, j)

        @pl.when(jnp.logical_and(s >= 1, s <= shards))
        def _():
            ready(1, j)

        flags[0] = masks[0, j].astype(jnp.float32).astype(jnp.bfloat16)

        @pl.when(s > 0)
        def _():
            flags[1] = masks[1, j].astype(jnp.float32).astype(jnp.bfloat16)

        landed(s).wait()

        @pl.when(s == 0)
        def _():
            pl.semaphore_signal(pair_sem, inc=1, device_id=dev(peer), device_id_type=MESH)
            pl.semaphore_wait(pair_sem, 1)

            @pl.when(market == 1)
            def _():
                pl.delay(STAGGER)

        @pl.when(s > 0)
        def _():
            visit(1, s, j)

        @pl.when(s < stages)
        def _():
            visit(0, s, j)

        @pl.when(s < stages - 1)
        def _():
            hop(s).start()

        @pl.when(s == stages - 1)
        def _():
            home(s, base - 1).start()

    user_home().start()
    users_t[...] = users[core].T
    for m in range(2):
        @pl.when(market == m)
        def _():
            pltpu.make_async_copy(users_t, (ua_o, ub_o)[m], user_sem.at[5]).start()

    @pl.when(core == 1)
    def _():
        home(stages, base).start()

    def outs(src, m):
        return [pltpu.make_async_copy(src.at[c], (va_o, vb_o)[m].at[:, pl.ds(c * CHUNK, CHUNK)], out_sem.at[m, c])
                for c in range(chunks)]

    for m in range(2):
        mine = jnp.logical_and(core == 0, market == m)

        @pl.when(mine)
        def _():
            for cp in outs(items.at[stages], m):
                cp.start()

        @pl.when(jnp.logical_not(mine))
        def _():
            pltpu.make_async_copy(last_items.at[m], last_items.at[m], last_sem.at[m]).wait()
            for cp in outs(last_items.at[m], m):
                cp.start()

    user_home().wait()
    users_in[...] = users_out[...].T
    for m in range(2):
        @pl.when(market == m)
        def _():
            pltpu.make_async_copy(users_in, (ua_o, ub_o)[1 - m], user_sem.at[6]).start()
    pltpu.make_async_copy(users_t, users_t, user_sem.at[5]).wait()
    pltpu.make_async_copy(users_in, users_in, user_sem.at[6]).wait()
    for m in range(2):
        for cp in outs(last_items.at[m], m):
            cp.wait()
    user_push(0).wait_send()
    pltpu.make_async_copy(items.at[core], items.at[core], last_sem.at[2]).wait()

    @pl.loop(0, shards)
    def _(j):
        for kind, buf in ((0, rates), (1, masks)):
            pltpu.make_async_copy(buf.at[core, j], buf.at[core, j], push_sem.at[kind, j]).wait()

    @pl.loop(0, stages)
    def _(s):
        pltpu.make_async_copy(items.at[s], items.at[s], send_sem.at[s]).wait()

    @pl.when(core == 1)
    def _():
        home(stages, base).wait_send()


def place(ua, va, ub, vb, ua_o, va_o, ub_o, vb_o, sem):
    copies = [pltpu.make_async_copy(src, dst, sem.at[i])
              for i, (src, dst) in enumerate(((ua, ua_o), (va, va_o), (ub, ub_o), (vb, vb_o)))]
    for cp in copies:
        cp.start()
    for cp in copies:
        cp.wait()


def solution(mesh):
    shards = mesh.shape["shard"]
    row_spec = P(("rep", "shard"), None)

    def device_body(ratings_a, mask_a, users_a, items_a, ratings_b, mask_b, users_b, items_b):
        users_dev, rank = users_a.shape
        block = items_a.shape[0]
        chunks = block // CHUNK
        stages = EPOCHS * shards
        step_u = 0.5 * math.sqrt(rank) / (block + 2 * rank)
        step_v = 0.5 * math.sqrt(rank) / (users_dev + 2 * rank)
        hbm = pl.BlockSpec(memory_space=pltpu.HBM)
        vmem = pl.BlockSpec(memory_space=pltpu.VMEM)
        f32 = jnp.float32
        ut = jax.ShapeDtypeStruct((rank, users_dev), f32)
        vt = jax.ShapeDtypeStruct((rank, block), f32)
        outs = pl.pallas_call(
            functools.partial(kernel, shards, step_u, step_v),
            out_shape=(ut, vt, ut, vt),
            in_specs=[hbm] * 8,
            out_specs=[hbm] * 4,
            scratch_shapes=[
                pltpu.VMEM((2, shards, users_dev, block), f32),
                pltpu.VMEM((2, shards, users_dev, block), jnp.int32),
                pltpu.VMEM((2, users_dev, block), jnp.bfloat16),
                pltpu.VMEM((stages + 1, chunks, rank, CHUNK), f32),
                pltpu.VMEM((2, chunks, rank, CHUNK), f32),
                pltpu.VMEM((2, users_dev, rank), f32),
                pltpu.VMEM((rank, users_dev), f32),
                pltpu.VMEM((rank, users_dev), f32),
                pltpu.VMEM((users_dev, rank), f32),
                pltpu.SemaphoreType.DMA((2, 2, shards)),
                pltpu.SemaphoreType.DMA((2, shards)),
                pltpu.SemaphoreType.DMA((stages + 1,)),
                pltpu.SemaphoreType.DMA((stages + 1,)),
                pltpu.SemaphoreType.DMA((3,)),
                pltpu.SemaphoreType.DMA((7,)),
                pltpu.SemaphoreType.DMA((2, chunks)),
                pltpu.SemaphoreType.REGULAR,
                pltpu.SemaphoreType.REGULAR,
            ],
            compiler_params=pltpu.CompilerParams(
                collective_id=0, has_side_effects=True, vmem_limit_bytes=60 * 1024 * 1024),
            name="sweep_ring",
        )(ratings_a, mask_a, users_a.T, items_a.T, ratings_b, mask_b, users_b.T, items_b.T)
        outs = pl.pallas_call(
            place,
            out_shape=(ut, vt, ut, vt),
            in_specs=[vmem] * 4,
            out_specs=[pl.BlockSpec(memory_space=pl.ANY)] * 4,
            scratch_shapes=[pltpu.SemaphoreType.DMA((4,))],
            compiler_params=pltpu.CompilerParams(vmem_limit_bytes=60 * 1024 * 1024),
            name="place",
        )(*outs)
        return tuple(o.T for o in outs)

    return jax.shard_map(device_body, mesh=mesh, in_specs=(row_spec,) * 8, out_specs=(row_spec,) * 4, check_vma=False)
```

```python
import functools
import math
import jax
import jax.numpy as jnp
from jax import lax
from jax.experimental import pallas as pl
from jax.experimental.pallas import tpu as pltpu
from jax.sharding import PartitionSpec as P

SWEEP_STEPS = 4
EPOCHS = 2
WEIGHT_DECAY = 0.05
CHUNK = 256
AHEAD = 2
MESH = pl.DeviceIdType.MESH


def sweep(u_ref, v_ref, rate_ref, flag_ref, step_u, step_v):
    chunks = range(v_ref.shape[0])
    f32, bf16 = jnp.float32, jnp.bfloat16
    user = u_ref[...]
    user_low = user.astype(bf16)
    user_low_t = user.T.astype(bf16)
    item_low = [v_ref[c].astype(bf16) for c in chunks]
    approx = [jnp.dot(user_low, item_low[c], preferred_element_type=f32) for c in chunks]
    err_low = []
    for c in chunks:
        cols = pl.ds(c * CHUNK, CHUNK)
        err_low.append((approx[c] - rate_ref[:, cols]).astype(bf16) * flag_ref[:, cols])
    part = [lax.dot_general(err_low[c], item_low[c], (((1,), (1,)), ((), ())), preferred_element_type=f32) for c in chunks]
    grad_v = [jnp.dot(user_low_t, err_low[c], preferred_element_type=f32) for c in chunks]
    for c in chunks:
        item = v_ref[c]
        v_ref[c] = item - step_v * (grad_v[c] + WEIGHT_DECAY * item)
    grad_u = (part[0] + part[1]) + (part[2] + part[3])
    u_ref[...] = user - step_u * (grad_u + WEIGHT_DECAY * user)


def kernel(shards, step_u, step_v, ra, ma, ua, va, rb, mb, ub, vb, ua_o, va_o, ub_o, vb_o,
           rates, masks, flags, items, users, users_t, load_sem, first_sem, send_sem, recv_sem, out_sem, user_sem):
    me = lax.axis_index("shard")
    left = lax.rem(me + shards - 1, shards)
    right = lax.rem(me + 1, shards)
    block = rates.shape[-1]
    chunks = block // CHUNK
    stages = EPOCHS * shards
    rate_in, mask_in = (ra, rb), (ma, mb)

    def loads(m, t):
        j = lax.rem(me + t, shards)
        cols = pl.ds(pl.multiple_of(j * block, block), block)
        return (pltpu.make_async_copy(rate_in[m].at[:, cols], rates.at[m, j], load_sem.at[0, m, j]),
                pltpu.make_async_copy(mask_in[m].at[:, cols], masks.at[m, j], load_sem.at[1, m, j]))

    def first(m, c):
        return pltpu.make_async_copy((va, vb)[m].at[:, pl.ds(c * CHUNK, CHUNK)], items.at[m, 0, c], first_sem.at[m, c])

    def last(m, c):
        return pltpu.make_async_copy(items.at[m, stages, c], (va_o, vb_o)[m].at[:, pl.ds(c * CHUNK, CHUNK)], out_sem.at[m, c])

    def hop(m, t):
        return pltpu.make_async_remote_copy(
            src_ref=items.at[m, t], dst_ref=items.at[m, t + 1], send_sem=send_sem.at[m, t],
            recv_sem=recv_sem.at[m, t + 1], device_id={"shard": left}, device_id_type=MESH)

    def user_in(m):
        return pltpu.make_async_copy((ua, ub)[m], users_t.at[m], user_sem.at[m])

    def user_out(m):
        return pltpu.make_async_copy(users_t.at[m], (ua_o, ub_o)[m], user_sem.at[m])

    for m in range(2):
        for c in range(chunks):
            first(m, c).start()
        user_in(m).start()
        for cp in loads(m, 0):
            cp.start()

    barrier = pltpu.get_barrier_semaphore()
    for other in (left, right):
        pl.semaphore_signal(barrier, inc=1, device_id={"shard": other}, device_id_type=MESH)

    for t in range(1, AHEAD):
        for m in range(2):
            for cp in loads(m, t):
                cp.start()

    for m in range(2):
        user_in(m).wait()
        users[m] = users_t[m].T
        for c in range(chunks):
            first(m, c).wait()

    @pl.loop(0, stages)
    def _(t):
        j = lax.rem(me + t, shards)

        @pl.when(t + AHEAD < shards)
        def _():
            for m in range(2):
                for cp in loads(m, t + AHEAD):
                    cp.start()
        for m in range(2):
            @pl.when(t < shards)
            def _():
                for cp in loads(m, t):
                    cp.wait()
            flags[m] = masks[m, j].astype(jnp.float32).astype(jnp.bfloat16)
        for m in range(2):
            @pl.when(t > 0)
            def _():
                hop(m, t - 1).wait_recv()

            for _ in range(SWEEP_STEPS):
                sweep(users.at[m], items.at[m, t], rates.at[m, j], flags.at[m], step_u, step_v)
            if m == 0:
                @pl.when(t == 0)
                def _():
                    pl.semaphore_wait(barrier, 2)
            hop(m, t).start()

    for m in range(2):
        users_t[m] = users[m].T
    for m in range(2):
        user_out(m).start()

    @pl.loop(0, stages - 1)
    def _(t):
        for m in range(2):
            hop(m, t).wait_send()

    for m in range(2):
        hop(m, stages - 1).wait_recv()
        for c in range(chunks):
            last(m, c).start()
    for m in range(2):
        for c in range(chunks):
            last(m, c).wait()
        user_out(m).wait()

    for m in range(2):
        hop(m, stages - 1).wait_send()


def place(ua, va, ub, vb, ua_o, va_o, ub_o, vb_o, sem):
    copies = [pltpu.make_async_copy(src, dst, sem.at[i])
              for i, (src, dst) in enumerate(((ua, ua_o), (va, va_o), (ub, ub_o), (vb, vb_o)))]
    for cp in copies:
        cp.start()
    for cp in copies:
        cp.wait()


def solution(mesh):
    shards = mesh.shape["shard"]
    row_spec = P(("rep", "shard"), None)

    def device_body(ratings_a, mask_a, users_a, items_a, ratings_b, mask_b, users_b, items_b):
        users_dev, rank = users_a.shape
        block = items_a.shape[0]
        chunks = block // CHUNK
        stages = EPOCHS * shards
        step_u = 0.5 * math.sqrt(rank) / (block + 2 * rank)
        step_v = 0.5 * math.sqrt(rank) / (users_dev + 2 * rank)
        hbm = pl.BlockSpec(memory_space=pltpu.HBM)
        vmem = pl.BlockSpec(memory_space=pltpu.VMEM)
        f32 = jnp.float32
        ut = jax.ShapeDtypeStruct((rank, users_dev), f32)
        vt = jax.ShapeDtypeStruct((rank, block), f32)
        outs = pl.pallas_call(
            functools.partial(kernel, shards, step_u, step_v),
            out_shape=(ut, vt, ut, vt),
            in_specs=[hbm] * 8,
            out_specs=[hbm] * 4,
            scratch_shapes=[
                pltpu.VMEM((2, shards, users_dev, block), f32),
                pltpu.VMEM((2, shards, users_dev, block), jnp.int32),
                pltpu.VMEM((2, users_dev, block), jnp.bfloat16),
                pltpu.VMEM((2, stages + 1, chunks, rank, CHUNK), f32),
                pltpu.VMEM((2, users_dev, rank), f32),
                pltpu.VMEM((2, rank, users_dev), f32),
                pltpu.SemaphoreType.DMA((2, 2, shards)),
                pltpu.SemaphoreType.DMA((2, chunks)),
                pltpu.SemaphoreType.DMA((2, stages)),
                pltpu.SemaphoreType.DMA((2, stages + 1)),
                pltpu.SemaphoreType.DMA((2, chunks)),
                pltpu.SemaphoreType.DMA((2,)),
            ],
            compiler_params=pltpu.CompilerParams(
                collective_id=0, has_side_effects=True, vmem_limit_bytes=60 * 1024 * 1024),
            name="sweep_ring",
        )(ratings_a, mask_a, users_a.T, items_a.T, ratings_b, mask_b, users_b.T, items_b.T)
        outs = pl.pallas_call(
            place,
            out_shape=(ut, vt, ut, vt),
            in_specs=[vmem] * 4,
            out_specs=[pl.BlockSpec(memory_space=pl.ANY)] * 4,
            scratch_shapes=[pltpu.SemaphoreType.DMA((4,))],
            compiler_params=pltpu.CompilerParams(vmem_limit_bytes=60 * 1024 * 1024),
            name="place",
        )(*outs)
        return tuple(o.T for o in outs)

    return jax.shard_map(device_body, mesh=mesh, in_specs=(row_spec,) * 8, out_specs=(row_spec,) * 4, check_vma=False)
```

```python
import functools
import math
import jax
import jax.numpy as jnp
from jax import lax
from jax.experimental import pallas as pl
from jax.experimental.pallas import tpu as pltpu
from jax.sharding import PartitionSpec as P

SWEEP_STEPS = 4
EPOCHS = 2
WEIGHT_DECAY = 0.05
CHUNK = 256
AHEAD = 2
MESH = pl.DeviceIdType.MESH


def sweep(u_ref, v_ref, rate_ref, flag_ref, step_u, step_v):
    chunks = range(v_ref.shape[0])
    f32, bf16 = jnp.float32, jnp.bfloat16
    user = u_ref[...]
    user_low = user.astype(bf16)
    user_low_t = user.T.astype(bf16)
    item_low = [v_ref[c].astype(bf16) for c in chunks]
    approx = [jnp.dot(user_low, item_low[c], preferred_element_type=f32) for c in chunks]
    err_low = []
    for c in chunks:
        cols = pl.ds(c * CHUNK, CHUNK)
        err_low.append((approx[c] - rate_ref[:, cols]).astype(bf16) * flag_ref[:, cols])
    part = [lax.dot_general(err_low[c], item_low[c], (((1,), (1,)), ((), ())), preferred_element_type=f32) for c in chunks]
    grad_v = [jnp.dot(user_low_t, err_low[c], preferred_element_type=f32) for c in chunks]
    for c in chunks:
        item = v_ref[c]
        v_ref[c] = item - step_v * (grad_v[c] + WEIGHT_DECAY * item)
    grad_u = (part[0] + part[1]) + (part[2] + part[3])
    u_ref[...] = user - step_u * (grad_u + WEIGHT_DECAY * user)


def kernel(shards, step_u, step_v, ra, ma, ua, va, rb, mb, ub, vb, ua_o, va_o, ub_o, vb_o,
           rates, masks, flags, items, users, users_t, load_sem, first_sem, send_sem, recv_sem, out_sem, user_sem):
    me = lax.axis_index("shard")
    left = lax.rem(me + shards - 1, shards)
    right = lax.rem(me + 1, shards)
    block = rates.shape[-1]
    chunks = block // CHUNK
    stages = EPOCHS * shards
    rate_in, mask_in = (ra, rb), (ma, mb)

    def loads(m, t):
        j = lax.rem(me + t, shards)
        cols = pl.ds(pl.multiple_of(j * block, block), block)
        return (pltpu.make_async_copy(rate_in[m].at[:, cols], rates.at[m, j], load_sem.at[0, m, j]),
                pltpu.make_async_copy(mask_in[m].at[:, cols], masks.at[m, j], load_sem.at[1, m, j]))

    def first(m, c):
        return pltpu.make_async_copy((va, vb)[m].at[:, pl.ds(c * CHUNK, CHUNK)], items.at[m, 0, c], first_sem.at[m, c])

    def last(m, c):
        return pltpu.make_async_copy(items.at[m, stages, c], (va_o, vb_o)[m].at[:, pl.ds(c * CHUNK, CHUNK)], out_sem.at[m, c])

    def hop(m, t):
        return pltpu.make_async_remote_copy(
            src_ref=items.at[m, t], dst_ref=items.at[m, t + 1], send_sem=send_sem.at[m, t],
            recv_sem=recv_sem.at[m, t + 1], device_id={"shard": left}, device_id_type=MESH)

    def user_in(m):
        return pltpu.make_async_copy((ua, ub)[m], users_t.at[m], user_sem.at[m])

    def user_out(m):
        return pltpu.make_async_copy(users_t.at[m], (ua_o, ub_o)[m], user_sem.at[m])

    for m in range(2):
        for c in range(chunks):
            first(m, c).start()
        user_in(m).start()
        for cp in loads(m, 0):
            cp.start()

    barrier = pltpu.get_barrier_semaphore()
    for other in (left, right):
        pl.semaphore_signal(barrier, inc=1, device_id={"shard": other}, device_id_type=MESH)

    for t in range(1, AHEAD):
        for m in range(2):
            for cp in loads(m, t):
                cp.start()

    for m in range(2):
        user_in(m).wait()
        users[m] = users_t[m].T
        for c in range(chunks):
            first(m, c).wait()

    @pl.loop(0, stages)
    def _(t):
        j = lax.rem(me + t, shards)

        @pl.when(t + AHEAD < shards)
        def _():
            for m in range(2):
                for cp in loads(m, t + AHEAD):
                    cp.start()
        for m in range(2):
            @pl.when(t < shards)
            def _():
                for cp in loads(m, t):
                    cp.wait()
            flags[m] = masks[m, j].astype(jnp.float32).astype(jnp.bfloat16)
        for m in range(2):
            @pl.when(t > 0)
            def _():
                hop(m, t - 1).wait_recv()

            for _ in range(SWEEP_STEPS):
                sweep(users.at[m], items.at[m, t], rates.at[m, j], flags.at[m], step_u, step_v)
            if m == 0:
                @pl.when(t == 0)
                def _():
                    pl.semaphore_wait(barrier, 2)
            hop(m, t).start()

    for m in range(2):
        users_t[m] = users[m].T
    for m in range(2):
        user_out(m).start()

    @pl.loop(0, stages - 1)
    def _(t):
        for m in range(2):
            hop(m, t).wait_send()

    for m in range(2):
        hop(m, stages - 1).wait_recv()
        for c in range(chunks):
            last(m, c).start()
    for m in range(2):
        for c in range(chunks):
            last(m, c).wait()
        user_out(m).wait()

    for m in range(2):
        hop(m, stages - 1).wait_send()


def place(ua, va, ub, vb, ua_o, va_o, ub_o, vb_o, ua_t, va_t, ub_t, vb_t, sem):
    route = ((ua, ua_t, ua_o), (va, va_t, va_o), (ub, ub_t, ub_o), (vb, vb_t, vb_o))
    loads = [pltpu.make_async_copy(src, mid, sem.at[0, i]) for i, (src, mid, _) in enumerate(route)]
    stores = [pltpu.make_async_copy(mid, dst, sem.at[1, i]) for i, (_, mid, dst) in enumerate(route)]
    for cp in loads:
        cp.start()
    for load, store in zip(loads, stores):
        load.wait()
        store.start()
    for cp in stores:
        cp.wait()


def solution(mesh):
    shards = mesh.shape["shard"]
    row_spec = P(("rep", "shard"), None)

    def device_body(ratings_a, mask_a, users_a, items_a, ratings_b, mask_b, users_b, items_b):
        users_dev, rank = users_a.shape
        block = items_a.shape[0]
        chunks = block // CHUNK
        stages = EPOCHS * shards
        step_u = 0.5 * math.sqrt(rank) / (block + 2 * rank)
        step_v = 0.5 * math.sqrt(rank) / (users_dev + 2 * rank)
        hbm = pl.BlockSpec(memory_space=pltpu.HBM)
        f32 = jnp.float32
        ut = jax.ShapeDtypeStruct((rank, users_dev), f32)
        vt = jax.ShapeDtypeStruct((rank, block), f32)
        outs = pl.pallas_call(
            functools.partial(kernel, shards, step_u, step_v),
            out_shape=(ut, vt, ut, vt),
            in_specs=[hbm] * 8,
            out_specs=[hbm] * 4,
            scratch_shapes=[
                pltpu.VMEM((2, shards, users_dev, block), f32),
                pltpu.VMEM((2, shards, users_dev, block), jnp.int32),
                pltpu.VMEM((2, users_dev, block), jnp.bfloat16),
                pltpu.VMEM((2, stages + 1, chunks, rank, CHUNK), f32),
                pltpu.VMEM((2, users_dev, rank), f32),
                pltpu.VMEM((2, rank, users_dev), f32),
                pltpu.SemaphoreType.DMA((2, 2, shards)),
                pltpu.SemaphoreType.DMA((2, chunks)),
                pltpu.SemaphoreType.DMA((2, stages)),
                pltpu.SemaphoreType.DMA((2, stages + 1)),
                pltpu.SemaphoreType.DMA((2, chunks)),
                pltpu.SemaphoreType.DMA((2,)),
            ],
            compiler_params=pltpu.CompilerParams(
                collective_id=0, has_side_effects=True, vmem_limit_bytes=60 * 1024 * 1024),
            name="sweep_ring",
        )(ratings_a, mask_a, users_a.T, items_a.T, ratings_b, mask_b, users_b.T, items_b.T)
        outs = pl.pallas_call(
            place,
            out_shape=(ut, vt, ut, vt),
            in_specs=[hbm] * 4,
            out_specs=[hbm] * 4,
            scratch_shapes=[pltpu.VMEM((rank, users_dev), f32), pltpu.VMEM((rank, block), f32)] * 2 + [pltpu.SemaphoreType.DMA((2, 4))],
            compiler_params=pltpu.CompilerParams(vmem_limit_bytes=60 * 1024 * 1024),
            name="place",
        )(*outs)
        return tuple(o.T for o in outs)

    return jax.shard_map(device_body, mesh=mesh, in_specs=(row_spec,) * 8, out_specs=(row_spec,) * 4, check_vma=False)
```
